128 devices in a mesh: grp: 2 (over z_lo), ang: 64 (over z_hi, x, y, core).
Axes of the slice: x: 4, y: 4, z: 4 (z_hi: 2, z_lo: 2; z = z_hi * 2 + z_lo), core: 2. Of those that a mesh axis runs over, the one named last changes fastest.
Arguments:
- children: bfloat16 [2, 128, 8, 2, 1, 8192], P(None, ('grp', 'ang')), may hold values from -6 to 6
- present: int32 [128, 8], P(('grp', 'ang')), may hold values 0 or 1
- interp: float32 [8, 32768], replicated, may hold values from -2 to 2
- phase: float32 [8, 32768], replicated, may hold values from -3.140625 to 3.140625
- trans: float32 [2, 316, 32768], P(None, None, 'ang'), may hold values from -0.6 to 0.6
- sources: int32 [128, 8], P('grp'), may hold values from 0 to 127
- trans_ids: int32 [128, 8], P('grp'), may hold values from 0 to 315
- list_len: int32 [128], P('grp'), may hold values from 1 to 8
Outputs:
- received: float32 [2, 128, 2, 1, 32768], P(None, 'grp', None, None, 'ang')
The draws below stay inside these ranges and needn't reach their ends.
All inputs are finite; a program needn't handle non-finite values. No bound on the sum of `present` on one device may be relied on, other than what follows from the above.
Results may differ from the reference program's by a relative error of at most 0.0029.
Values may be sent and summed in bfloat16 or wider, within the bound.
No kernel may reach another device: no remote copies, remote signals or barrier semaphores. Data moves between devices by JAX's collectives and lax.ppermute only.
A program may use at most 128 MiB of HBM per device.

```python
import jax
import jax.numpy as jnp
from jax import lax

HW = 4
POL = 2
CH = 8
R = 1
LIST = 8
NT = 316
TAPS = 8
K = 32768
KC = 8192
CLUSTERS = 128


def touch_ends(values, stream_key, low, largest):
    spot = [jax.random.randint(jax.random.fold_in(stream_key, axis), (), 0, length) for axis, length in enumerate(values.shape)]
    main_axis = values.shape.index(max(values.shape))
    next_to = spot[:main_axis] + [(spot[main_axis] + 1) % values.shape[main_axis]] + spot[main_axis + 1:]
    return values.at[tuple(spot)].set(low).at[tuple(next_to)].set(largest)


def levels(stream_key, dims, shards, smallest, high):
    gain, own = 1.0, jax.random.fold_in(stream_key, 6)
    for dim, parts in shards:
        draws = jnp.exp(jax.random.uniform(jax.random.fold_in(own, dim), (parts,), jnp.float32, smallest / len(shards), high / len(shards)))
        gain = gain * jnp.repeat(draws, dims[dim] // parts).reshape([-1 if axis == dim else 1 for axis in range(len(dims))])
    return gain


def normal_values(rng, shape, scale, most, shards=(), held_as=jnp.bfloat16):
    array = scale * jax.random.normal(rng, shape, jnp.float32)
    if shards:
        array = array * levels(rng, shape, shards, -0.22, 0.18)
    return jnp.clip(array, -most, most).astype(held_as)


def setup_inputs(seed: int = 0) -> dict:
    key_list = jax.random.split(jax.random.key(seed), 9)
    return {
        "children": normal_values(key_list[0], (2, CLUSTERS, CH, POL, R, KC), 1.0, 6.0, ((1, 128),)),
        "present": touch_ends((jax.random.randint(key_list[1], (CLUSTERS, CH), 0, 4) < 3).astype(jnp.int32), jax.random.fold_in(key_list[1], 1), 0, 1),
        "interp": normal_values(key_list[2], (TAPS, K), TAPS ** -0.5, 2.0, (), jnp.float32),
        "phase": jnp.clip(jax.random.uniform(key_list[3], (CH, K), jnp.float32, -3.140625, 3.140625), -3.140625, 3.140625),
        "trans": normal_values(key_list[4], (2, NT, K), 0.1, 0.6, ((2, 64),), jnp.float32),
        "sources": touch_ends(jax.random.randint(key_list[5], (CLUSTERS, LIST), 0, CLUSTERS), jax.random.fold_in(key_list[5], 1), 0, CLUSTERS - 1).astype(jnp.int32),
        "trans_ids": touch_ends(jax.random.randint(key_list[6], (CLUSTERS, LIST), 0, NT), jax.random.fold_in(key_list[6], 1), 0, NT - 1).astype(jnp.int32),
        "list_len": touch_ends(jax.random.randint(key_list[7], (CLUSTERS,), 1, LIST + 1), jax.random.fold_in(key_list[7], 1), 1, LIST).astype(jnp.int32),
    }


def aggregate(extended, weights, cosine, sine_part, coarse_len):
    taps_count = weights.shape[0]
    octants = extended.shape[2]
    fine_len = 4 * coarse_len
    real_acc = None
    imag_acc = None
    for octant in range(octants):
        spread = jnp.repeat(extended[:, :, octant].astype(jnp.float32), 4, axis=-1)
        refined = jnp.zeros(spread.shape[:-1] + (fine_len,), jnp.float32)
        for stencil in range(taps_count):
            window = spread[..., 4 * stencil:4 * stencil + fine_len]
            refined = refined + window * weights[stencil]
        cos_row = cosine[octant]
        sin_row = sine_part[octant]
        real_term = refined[0] * cos_row - refined[1] * sin_row
        imag_term = refined[0] * sin_row + refined[1] * cos_row
        if real_acc is None:
            real_acc = jnp.zeros_like(real_term) + real_term
            imag_acc = jnp.zeros_like(imag_term) + imag_term
        else:
            real_acc = real_acc + real_term
            imag_acc = imag_acc + imag_term
    return jnp.stack([real_acc, imag_acc]).astype(jnp.bfloat16)


def reference(children, present, interp, phase, trans, sources, trans_ids, list_len):
    cosine = jnp.cos(phase)
    sine_part = jnp.sin(phase)
    coarse_len = children.shape[-1]

    def one_parent(pair):
        kept_children = pair[0] * pair[1].astype(jnp.bfloat16)[None, :, None, None, None]
        extended = jnp.concatenate([kept_children[..., -HW:], kept_children, kept_children[..., :HW]], axis=-1)
        return aggregate(extended[:, None], interp, cosine, sine_part, coarse_len)[:, 0]

    parents = lax.map(one_parent, (jnp.moveaxis(children, 1, 0), present))
    parents = jnp.moveaxis(parents, 0, 1)

    def one_receiver(triple):
        source_ids, operator_ids, used = triple
        real_sum = jnp.zeros(parents.shape[2:], jnp.float32)
        imag_sum = jnp.zeros(parents.shape[2:], jnp.float32)
        for position in range(LIST):
            source_rows = parents[:, source_ids[position]].astype(jnp.float32)
            operator_cols = trans[:, operator_ids[position]][:, None, None, :]
            active = (position < used).astype(jnp.float32)
            real_sum = real_sum + active * (operator_cols[0] * source_rows[0] - operator_cols[1] * source_rows[1])
            imag_sum = imag_sum + active * (operator_cols[0] * source_rows[1] + operator_cols[1] * source_rows[0])
        return jnp.stack([real_sum, imag_sum])

    result = lax.map(one_receiver, (sources, trans_ids, list_len))
    return jnp.moveaxis(result, 0, 1)
```

```python
import functools

import jax
import jax.numpy as jnp
from jax import lax
from jax.experimental import pallas as pl
from jax.experimental.pallas import tpu as pltpu
from jax.sharding import PartitionSpec as P

HW = 4
LANES = 128
F32 = jnp.float32
BF16 = jnp.bfloat16

SIN_TERMS = (-0.1666666567325592, 0.008333242498338223, -0.00019822783360723406, 2.634888232933008e-06)
COS_TERMS = (0.0416666679084301, -0.0013888812391087413, 2.4786117137409747e-05, -2.6547101583673793e-07)


def horner(terms, z):
    total = jnp.full_like(z, terms[-1])
    for term in terms[-2::-1]:
        total = total * z + term
    return total


def sin_cos(angle):
    half = angle * 0.5
    z = half * half
    sin_half = half + (half * z) * horner(SIN_TERMS, z)
    cos_half = (1.0 - 0.5 * z) + (z * z) * horner(COS_TERMS, z)
    twice = sin_half + sin_half
    return twice * cos_half, 1.0 - twice * sin_half


def row_sums(rows):
    place = lax.broadcasted_iota(jnp.int32, rows[0].shape, 0)
    for distance in (1, 2, 4):
        first = (place & distance) == 0
        rows = [
            jnp.where(first, a, b) + pltpu.roll(jnp.where(first, b, a), distance, 0)
            for a, b in zip(rows[0::2], rows[1::2])
        ]
    return rows[0]


def aggregate_kernel(blocks, total, present_ref, children_ref, interp_ref, phase_ref, out_ref):
    step = pl.program_id(0)
    lane = lax.broadcasted_iota(jnp.int32, (8, LANES), 1)
    row = lax.broadcasted_iota(jnp.int32, (8, LANES), 0)
    kept = jnp.zeros((8, LANES), F32)
    for octant in range(8):
        kept = jnp.where(row == octant, present_ref[0, octant].astype(F32), kept)
    kept = jnp.concatenate([kept] * 4, axis=0)
    lane32 = lax.broadcasted_iota(jnp.int32, (32, LANES), 1)
    fine_lane = lax.broadcasted_iota(jnp.int32, (8, 4 * LANES), 1)
    bits = [((fine_lane // 4) & d) != 0 for d in (1, 2, 4)]
    row16 = lax.broadcasted_iota(jnp.int32, (16, LANES), 0)
    lane16 = lax.broadcasted_iota(jnp.int32, (16, LANES), 1) // 4
    bands = []
    for i in range(3):
        tap = row16 + 16 * i - lane16
        bands.append(jnp.where((tap >= 0) & (tap < 8), 1.0, 0.0).astype(BF16))
    nothing = jnp.zeros((16, LANES), BF16)

    for i in range(blocks):
        a = step * blocks + i

        def coarse(index):
            at = pl.multiple_of(index * LANES, LANES)
            return children_ref[:, pl.ds(at, LANES)].astype(F32) * kept

        before = coarse(lax.rem(a + total - 1, total))
        here = coarse(a)
        after = coarse(lax.rem(a + 1, total))
        windows = (
            jnp.where(lane32 < HW, pltpu.roll(before, HW, 1), pltpu.roll(here, HW, 1)).astype(BF16),
            jnp.where(lane32 < 64 + HW, pltpu.roll(here, 64 + HW, 1), pltpu.roll(after, 64 + HW, 1)).astype(BF16),
        )
        fine = pl.ds(4 * LANES * i, 4 * LANES)
        turned = interp_ref[:, fine]
        for bit, distance in zip(bits, (1, 2, 4)):
            turned = jnp.where(bit, pltpu.roll(turned, distance, 0), turned)
        turned = jnp.concatenate([turned, turned], axis=0)
        high = turned.astype(BF16)
        low = (turned - high.astype(F32)).astype(BF16)
        sine, cosine = sin_cos(phase_ref[:, fine])
        real = [None] * 8
        imag = [None] * 8
        for half in range(2):
            weights = []
            for part in (high, low):
                left = part[:, (2 * half) * LANES : (2 * half + 1) * LANES]
                right = part[:, (2 * half + 1) * LANES : (2 * half + 2) * LANES]
                weights.append(
                    jnp.concatenate(
                        [
                            jnp.concatenate([left * b for b in bands] + [nothing] * 5, axis=0),
                            jnp.concatenate([nothing] * 2 + [right * b for b in bands] + [nothing] * 3, axis=0),
                        ],
                        axis=1,
                    )
                )
            refined = jnp.dot(
                jnp.concatenate([windows[half], windows[half]], axis=1),
                jnp.concatenate(weights, axis=0),
                preferred_element_type=F32,
            )
            for tile in range(2):
                at = (2 * half + tile) * LANES
                cos_tile = cosine[:, at : at + LANES]
                sin_tile = sine[:, at : at + LANES]
                for pol in range(2):
                    re = refined[8 * pol : 8 * pol + 8, tile * LANES : (tile + 1) * LANES]
                    im = refined[16 + 8 * pol : 24 + 8 * pol, tile * LANES : (tile + 1) * LANES]
                    spot = 2 * (2 * half + tile) + pol
                    real[spot] = re * cos_tile - im * sin_tile
                    imag[spot] = re * sin_tile + im * cos_tile
        pattern = jnp.concatenate([row_sums(real), row_sums(imag)], axis=0).astype(BF16)
        for group in range(out_ref.shape[0]):
            out_ref[group, i] = pattern


def translate_kernel(
    receivers, sources_ref, ids_ref, used_ref, pattern_ref, trans_ref, out_ref, unpacked
):
    step = pl.program_id(0)
    clusters = pattern_ref.shape[0]
    slots = sources_ref.shape[0]

    @pl.when(step == 0)
    def _():
        def unpack(c, carry):
            unpacked[c] = pattern_ref[c].astype(F32)
            return carry

        lax.fori_loop(0, clusters, unpack, 0, unroll=8)
        unpacked[clusters] = jnp.zeros((16, LANES), F32)

    row = lax.broadcasted_iota(jnp.int32, (8, LANES), 0)
    even = (row & 1) == 0
    order = 2 * (row & 3) + (row >> 2)

    def receive(c, carry):
        receiver = step * receivers + c
        used = used_ref[receiver]
        real = jnp.zeros((8, LANES), F32)
        imag = jnp.zeros((8, LANES), F32)
        for slot in range(slots):
            source = jnp.where(slot < used, sources_ref[slot, receiver], clusters)
            operator = trans_ref[ids_ref[slot, receiver]]
            values = unpacked[source]
            re, im = values[:8], values[8:]
            t_re = jnp.where(even, operator, pltpu.roll(operator, 1, 0))
            t_im = jnp.where(even, pltpu.roll(operator, 7, 0), operator)
            real = real + (t_re * re - t_im * im)
            imag = imag + (t_re * im + t_im * re)
        out_ref[0, c] = jnp.take_along_axis(real, order, axis=0)
        out_ref[1, c] = jnp.take_along_axis(imag, order, axis=0)
        return carry

    lax.fori_loop(0, receivers, receive, 0, unroll=4)


def aggregate(children, present, interp, phase, copies):
    rows, coarse_len = children.shape
    fine_len = interp.shape[1]
    total = coarse_len // LANES
    steps = 8
    blocks = total // steps
    return pl.pallas_call(
        functools.partial(aggregate_kernel, blocks, total),
        grid=(steps,),
        in_specs=[
            pl.BlockSpec(memory_space=pltpu.SMEM),
            pl.BlockSpec((rows, coarse_len), lambda s: (0, 0)),
            pl.BlockSpec((8, fine_len // steps), lambda s: (0, s)),
            pl.BlockSpec((8, fine_len // steps), lambda s: (0, s)),
        ],
        out_specs=pl.BlockSpec((copies, blocks, 16, LANES), lambda s: (0, s, 0, 0)),
        out_shape=jax.ShapeDtypeStruct((copies, total, 16, LANES), BF16),
        name="aggregate",
    )(present, children, interp, phase)


def translate(sources, ids, used, pattern, trans):
    slots, local = sources.shape
    clusters = pattern.shape[0]
    steps = 4
    receivers = local // steps
    return pl.pallas_call(
        functools.partial(translate_kernel, receivers),
        grid=(steps,),
        in_specs=[
            pl.BlockSpec(memory_space=pltpu.SMEM),
            pl.BlockSpec(memory_space=pltpu.SMEM),
            pl.BlockSpec(memory_space=pltpu.SMEM),
            pl.BlockSpec((clusters, 16, LANES), lambda s: (0, 0, 0)),
            pl.BlockSpec(trans.shape, lambda s: (0, 0, 0)),
        ],
        out_specs=pl.BlockSpec((2, receivers, 8, LANES), lambda s: (0, s, 0, 0)),
        out_shape=jax.ShapeDtypeStruct((2, local, 8, LANES), F32),
        scratch_shapes=[pltpu.VMEM((clusters + 1, 16, LANES), F32)],
        name="translate",
    )(sources, ids, used, pattern, trans)


def local(children, present, interp, phase, trans, sources, trans_ids, list_len):
    groups = lax.axis_size("grp")
    rows = jnp.transpose(children[:, 0, :, :, 0], (0, 2, 1, 3)).reshape(32, -1)
    pattern = aggregate(rows, present, interp, phase, groups)
    pattern = lax.all_to_all(
        pattern.reshape(-1, 16, LANES), ("grp", "ang"), 0, 0, tiled=True
    )
    kinds = trans.shape[1]
    operators = jnp.transpose(
        jnp.transpose(trans, (1, 0, 2)).reshape(kinds, 2, 4, LANES), (0, 2, 1, 3)
    ).reshape(kinds, 8, LANES)
    out = translate(sources.T, trans_ids.T, list_len, pattern, operators)
    return out.reshape(2, -1, 2, 1, 4 * LANES)


def solution(mesh):
    placed = (
        P(None, ("grp", "ang"), None, None, None, None),
        P(("grp", "ang"), None),
        P(),
        P(),
        P(None, None, "ang"),
        P("grp", None),
        P("grp", None),
        P("grp"),
    )
    return jax.shard_map(
        local,
        mesh=mesh,
        in_specs=placed,
        out_specs=P(None, "grp", None, None, "ang"),
        check_vma=False,
    )
```

```python
import functools

import jax
import jax.numpy as jnp
from jax import lax
from jax.experimental import pallas as pl
from jax.experimental.pallas import tpu as pltpu
from jax.sharding import PartitionSpec as P

HW = 4
LANES = 128
CHUNK = 32
BATCH = 8
F32 = jnp.float32
BF16 = jnp.bfloat16
ROOT = 2.0**0.5

SIN_TERMS = tuple(
    ROOT * v * 0.5 ** (2 * i + 1)
    for i, v in enumerate((1.0, -0.1666666567325592, 0.008333242498338223, -0.00019822783360723406, 2.634888232933008e-06))
)
COS_TERMS = tuple(
    ROOT * v * 0.25**i
    for i, v in enumerate(
        (1.0, -0.5, 0.0416666679084301, -0.0013888812391087413, 2.4786117137409747e-05, -2.6547101583673793e-07)
    )
)


def horner(terms, z):
    total = z * terms[-1] + terms[-2]
    for term in terms[-3::-1]:
        total = total * z + term
    return total


def sin_cos(angle):
    z = angle * angle
    sin_half = angle * horner(SIN_TERMS, z)
    cos_half = horner(COS_TERMS, z)
    return sin_half * cos_half, 1.0 - sin_half * sin_half


def row_sums(rows):
    place = lax.broadcasted_iota(jnp.int32, rows[0].shape, 0)
    for distance in (1, 2, 4):
        first = (place & distance) == 0
        rows = [
            jnp.where(first, a, b) + pltpu.roll(jnp.where(first, b, a), distance, 0)
            for a, b in zip(rows[0::2], rows[1::2])
        ]
    return rows[0]


def aggregate_kernel(
    present_ref, children_ref, interp_ref, phase_ref, out_ref,
    stored, spread, weights_in, phase_in, patterns, flags, child_sem, flag_sem, weight_sem, phase_sem, out_sem,
):
    groups, total = out_ref.shape[:2]
    chunks = total // CHUNK
    span = 4 * LANES * CHUNK
    octants = 8
    parts = 2

    def weight_copy(c):
        at = pl.ds(pl.multiple_of(c * span, span), span)
        return pltpu.make_async_copy(interp_ref.at[:, at], weights_in.at[:, at], weight_sem.at[c])

    def phase_copy(c):
        at = pl.ds(pl.multiple_of(c * span, span), span)
        return pltpu.make_async_copy(phase_ref.at[:, at], phase_in.at[:, at], phase_sem.at[c])

    def out_copy(c, g):
        at = pl.ds(c * CHUNK, CHUNK)
        return pltpu.make_async_copy(patterns.at[at], out_ref.at[g, at], out_sem.at[c, g])

    child_copy = pltpu.make_async_copy(children_ref, stored, child_sem)
    child_copy.start()
    flag_copy = pltpu.make_async_copy(present_ref, flags, flag_sem)
    flag_copy.start()
    for c in range(chunks):
        weight_copy(c).start()
        phase_copy(c).start()
    flag_copy.wait()
    child_copy.wait()

    per = 2 * total
    for octant in range(octants):
        flag = flags[0, octant].astype(F32)
        for part in range(parts):

            def unpack(m, carry, flag=flag, octant=octant, part=part):
                at = pl.multiple_of((part * octants + octant) * per + 16 * m, 16)
                rows = stored[pl.ds(at, 16), :].astype(F32) * flag
                to = (part * per + 16 * m) * octants + octant
                spread[pl.ds(to, 8, stride=octants), :] = rows[:8]
                spread[pl.ds(to + 8 * octants, 8, stride=octants), :] = rows[8:]
                return carry

            lax.fori_loop(0, per // 16, unpack, 0, unroll=True)

    lane = lax.broadcasted_iota(jnp.int32, (8, LANES), 1)
    row = lax.broadcasted_iota(jnp.int32, (8, LANES), 0)
    turn = (row - lane // 4) & 7
    row16 = lax.broadcasted_iota(jnp.int32, (16, LANES), 0)
    lane16 = lax.broadcasted_iota(jnp.int32, (16, LANES), 1) // 4
    bands = []
    for i in range(3):
        tap = row16 + 16 * i - lane16
        bands.append(jnp.where((tap >= 0) & (tap < 8), 1.0, 0.0).astype(BF16))
    nothing = jnp.zeros((16, LANES), BF16)

    def coarse(index):
        return [
            spread[pl.ds(pl.multiple_of((part * per + 2 * index + pol) * octants, 8), 8), :]
            for part in range(parts)
            for pol in range(2)
        ]

    def chunk(c, carry):
        weight_copy(c).wait()
        phase_copy(c).wait()
        near, far = [], []
        for i in range(-1, CHUNK + 1):
            values = coarse(lax.rem(c * CHUNK + i + total, total))
            near.append([pltpu.roll(v, HW, 1) for v in values] if i < CHUNK else None)
            far.append([pltpu.roll(v, 64 + HW, 1) for v in values] if i >= 0 else None)
        for i in range(CHUNK):
            windows = (
                jnp.concatenate([jnp.where(lane < HW, b, h) for b, h in zip(near[i], near[i + 1])], axis=0).astype(BF16),
                jnp.concatenate([jnp.where(lane < 64 + HW, h, a) for h, a in zip(far[i + 1], far[i + 2])], axis=0).astype(BF16),
            )
            base = pl.multiple_of(c * span, span) + 4 * LANES * i
            real = [None] * 8
            imag = [None] * 8
            for half in range(2):
                high, low = [], []
                for tile in range(2):
                    at = pl.ds(base + (2 * half + tile) * LANES, LANES)
                    turned = jnp.take_along_axis(weights_in[:, at], turn, axis=0, mode="promise_in_bounds")
                    turned = jnp.concatenate([turned, turned], axis=0)
                    top = turned.astype(BF16)
                    high.append(top)
                    low.append((turned - top.astype(F32)).astype(BF16))
                weights = [
                    jnp.concatenate(
                        [
                            jnp.concatenate([left * b for b in bands] + [nothing] * 5, axis=0),
                            jnp.concatenate([nothing] * 2 + [right * b for b in bands] + [nothing] * 3, axis=0),
                        ],
                        axis=1,
                    )
                    for left, right in (high, low)
                ]
                refined = jnp.dot(
                    jnp.concatenate([windows[half], windows[half]], axis=1),
                    jnp.concatenate(weights, axis=0),
                    preferred_element_type=F32,
                )
                for tile in range(2):
                    at = pl.ds(base + (2 * half + tile) * LANES, LANES)
                    sin_tile, cos_tile = sin_cos(phase_in[:, at])
                    for pol in range(2):
                        re = refined[8 * pol : 8 * pol + 8, tile * LANES : (tile + 1) * LANES]
                        im = refined[16 + 8 * pol : 24 + 8 * pol, tile * LANES : (tile + 1) * LANES]
                        spot = 2 * (2 * half + tile) + pol
                        real[spot] = re * cos_tile - im * sin_tile
                        imag[spot] = re * sin_tile + im * cos_tile
            patterns[c * CHUNK + i] = jnp.concatenate([row_sums(real), row_sums(imag)], axis=0).astype(BF16)
        for g in range(groups):
            out_copy(c, g).start()
        return carry

    lax.fori_loop(0, chunks, chunk, 0)
    for c in range(chunks):
        for g in range(groups):
            out_copy(c, g).wait()


def aggregate(children, present, interp, phase, groups):
    total = children.shape[0] // 32
    chunks = total // CHUNK
    anywhere = pl.BlockSpec(memory_space=pl.ANY)
    return pl.pallas_call(
        aggregate_kernel,
        in_specs=[anywhere, anywhere, anywhere, anywhere],
        out_specs=anywhere,
        out_shape=jax.ShapeDtypeStruct((groups, total, 16, LANES), BF16),
        scratch_shapes=[
            pltpu.VMEM(children.shape, BF16),
            pltpu.VMEM(children.shape, F32),
            pltpu.VMEM(interp.shape, F32),
            pltpu.VMEM(phase.shape, F32),
            pltpu.VMEM((total, 16, LANES), BF16),
            pltpu.SMEM(present.shape, jnp.int32),
            pltpu.SemaphoreType.DMA,
            pltpu.SemaphoreType.DMA,
            pltpu.SemaphoreType.DMA((chunks,)),
            pltpu.SemaphoreType.DMA((chunks,)),
            pltpu.SemaphoreType.DMA((chunks, groups)),
        ],
        name="aggregate",
    )(present, children, interp, phase)


def aggregate_local(children, present, interp, phase, groups=2):
    total = children.shape[5] // LANES
    rows = jnp.transpose(children.reshape(2, 8, 2, total, LANES), (0, 1, 3, 2, 4)).reshape(-1, LANES)
    return aggregate(rows, present, interp, phase, groups)


def translate_kernel(
    sources_ref, ids_ref, used_ref, pattern_ref, trans_ref, out_ref, places, table, unpacked, received, table_sem, out_sem
):
    slots, receivers = sources_ref.shape
    clusters = pattern_ref.shape[0] // 16
    batches = receivers // BATCH

    def out_copy(b):
        at = pl.ds(b * BATCH, BATCH)
        return pltpu.make_async_copy(received.at[:, at], out_ref.at[:, at], out_sem.at[b])

    slot_row = lax.broadcasted_iota(jnp.int32, (slots, receivers), 0)
    places[:slots, :] = jnp.where(slot_row < used_ref[...], sources_ref[...], clusters) * 16
    places[slots:, :] = ids_ref[...] * 8
    table_copy = pltpu.make_async_copy(places, table, table_sem)
    table_copy.start()

    def unpack(c, carry):
        at = pl.ds(pl.multiple_of(16 * c, 16), 16)
        unpacked[at, :] = pattern_ref[at, :].astype(F32)
        return carry

    lax.fori_loop(0, clusters, unpack, 0, unroll=8)
    unpacked[pl.ds(16 * clusters, 16), :] = jnp.zeros((16, LANES), F32)
    row = lax.broadcasted_iota(jnp.int32, (8, LANES), 0)
    even = (row & 1) == 0
    order = 2 * (row & 3) + (row >> 2)
    table_copy.wait()

    for receiver in range(receivers):
        real = imag = None
        for slot in range(slots):
            source = pl.multiple_of(table[slot, receiver], 16)
            operator = trans_ref[pl.ds(pl.multiple_of(table[slots + slot, receiver], 8), 8), :]
            re = unpacked[pl.ds(source, 8), :]
            im = unpacked[pl.ds(source + 8, 8), :]
            t_re = jnp.where(even, operator, pltpu.roll(operator, 1, 0))
            t_im = jnp.where(even, pltpu.roll(operator, 7, 0), operator)
            new_re = t_re * re - t_im * im
            new_im = t_re * im + t_im * re
            real = new_re if real is None else real + new_re
            imag = new_im if imag is None else imag + new_im
        received[0, receiver] = jnp.take_along_axis(real, order, axis=0, mode="promise_in_bounds")
        received[1, receiver] = jnp.take_along_axis(imag, order, axis=0, mode="promise_in_bounds")
        if (receiver + 1) % BATCH == 0:
            out_copy(receiver // BATCH).start()
    for b in range(batches):
        out_copy(b).wait()


def translate_local(sources, trans_ids, list_len, pattern, trans):
    kinds = trans.shape[1]
    receivers, slots = sources.shape
    clusters = pattern.shape[0]
    operators = jnp.transpose(
        jnp.transpose(trans, (1, 0, 2)).reshape(kinds, 2, 4, LANES), (0, 2, 1, 3)
    ).reshape(kinds * 8, LANES)
    inside = pl.BlockSpec(memory_space=pltpu.VMEM)
    out = pl.pallas_call(
        translate_kernel,
        in_specs=[inside] * 5,
        out_specs=pl.BlockSpec(memory_space=pl.ANY),
        out_shape=jax.ShapeDtypeStruct((2, receivers, 8, LANES), F32),
        scratch_shapes=[
            pltpu.VMEM((2 * slots, receivers), jnp.int32),
            pltpu.SMEM((2 * slots, receivers), jnp.int32),
            pltpu.VMEM((16 * (clusters + 1), LANES), F32),
            pltpu.VMEM((2, receivers, 8, LANES), F32),
            pltpu.SemaphoreType.DMA,
            pltpu.SemaphoreType.DMA((receivers // BATCH,)),
        ],
        compiler_params=pltpu.CompilerParams(vmem_limit_bytes=16 * 2**20),
        name="translate",
    )(sources.T, trans_ids.T, list_len.reshape(1, -1), pattern.reshape(-1, LANES), operators)
    return out.reshape(2, -1, 2, 1, 4 * LANES)


def local(children, present, interp, phase, trans, sources, trans_ids, list_len):
    pattern = aggregate_local(children, present, interp, phase, lax.axis_size("grp"))
    pattern = lax.all_to_all(
        pattern.reshape(-1, 16, LANES), ("grp", "ang"), 0, 0, tiled=True
    )
    return translate_local(sources, trans_ids, list_len, pattern, trans)


def solution(mesh):
    placed = (
        P(None, ("grp", "ang"), None, None, None, None),
        P(("grp", "ang"), None),
        P(),
        P(),
        P(None, None, "ang"),
        P("grp", None),
        P("grp", None),
        P("grp"),
    )
    return jax.shard_map(
        local,
        mesh=mesh,
        in_specs=placed,
        out_specs=P(None, "grp", None, None, "ang"),
        check_vma=False,
    )
```

```python
import functools

import jax
import jax.numpy as jnp
from jax import lax
from jax.experimental import pallas as pl
from jax.experimental.pallas import tpu as pltpu
from jax.sharding import PartitionSpec as P

HW = 4
LANES = 128
CHUNK = 32
LIMIT = 57000
BATCH = 8
F32 = jnp.float32
BF16 = jnp.bfloat16
ROOT = 2.0**0.5

SIN_TERMS = tuple(
    ROOT * v * 0.5 ** (2 * i + 1)
    for i, v in enumerate((1.0, -0.1666666567325592, 0.008333242498338223, -0.00019822783360723406, 2.634888232933008e-06))
)
COS_TERMS = tuple(
    ROOT * v * 0.25**i
    for i, v in enumerate(
        (1.0, -0.5, 0.0416666679084301, -0.0013888812391087413, 2.4786117137409747e-05, -2.6547101583673793e-07)
    )
)


def horner(terms, z):
    total = z * terms[-1] + terms[-2]
    for term in terms[-3::-1]:
        total = total * z + term
    return total


def sin_cos(angle):
    z = angle * angle
    sin_half = angle * horner(SIN_TERMS, z)
    cos_half = horner(COS_TERMS, z)
    return sin_half * cos_half, 1.0 - sin_half * sin_half


def row_sums(rows):
    place = lax.broadcasted_iota(jnp.int32, rows[0].shape, 0)
    for distance in (1, 2, 4):
        first = (place & distance) == 0
        rows = [
            jnp.where(first, a, b) + pltpu.roll(jnp.where(first, b, a), distance, 0)
            for a, b in zip(rows[0::2], rows[1::2])
        ]
    return rows[0]


def aggregate_kernel(
    present_ref, children_ref, interp_ref, phase_ref, out_ref,
    stored, spread, weights_in, phase_in, flags, child_sem, flag_sem, weight_sem, phase_sem,
):
    groups, total = out_ref.shape[:2]
    chunks = total // CHUNK
    span = 4 * LANES * CHUNK
    octants = 8
    parts = 2
    per = 2 * total

    def weight_copy(c):
        at = pl.ds(pl.multiple_of(c * span, span), span)
        return pltpu.make_async_copy(interp_ref.at[:, at], weights_in.at[:, at], weight_sem.at[c])

    def phase_copy(c):
        at = pl.ds(pl.multiple_of(c * span, span), span)
        return pltpu.make_async_copy(phase_ref.at[:, at], phase_in.at[:, at], phase_sem.at[c])

    def child_copy(k):
        at = pl.ds(k * per, per)
        return pltpu.make_async_copy(children_ref.at[at], stored.at[at], child_sem.at[k])

    flag_copy = pltpu.make_async_copy(present_ref, flags, flag_sem)
    flag_copy.start()
    for k in range(parts * octants):
        child_copy(k).start()
    for c in range(chunks):
        weight_copy(c).start()
        phase_copy(c).start()
    flag_copy.wait()

    for octant in range(octants):
        flag = flags[0, octant].astype(F32)
        for part in range(parts):
            child_copy(part * octants + octant).wait()

            def unpack(m, carry, flag=flag, octant=octant, part=part):
                at = pl.multiple_of((part * octants + octant) * per + 16 * m, 16)
                rows = stored[pl.ds(at, 16), :].astype(F32) * flag
                to = (part * per + 16 * m) * octants + octant
                spread[pl.ds(to, 8, stride=octants), :] = rows[:8]
                spread[pl.ds(to + 8 * octants, 8, stride=octants), :] = rows[8:]
                return carry

            lax.fori_loop(0, per // 16, unpack, 0, unroll=True)

    lane = lax.broadcasted_iota(jnp.int32, (8, LANES), 1)
    row = lax.broadcasted_iota(jnp.int32, (8, LANES), 0)
    turn = (row - lane // 4) & 7
    row16 = lax.broadcasted_iota(jnp.int32, (16, LANES), 0)
    lane16 = lax.broadcasted_iota(jnp.int32, (16, LANES), 1) // 4
    bands = []
    for i in range(3):
        tap = row16 + 16 * i - lane16
        bands.append(jnp.where((tap >= 0) & (tap < 8), 1.0, 0.0).astype(BF16))
    lane_16 = lax.broadcasted_iota(jnp.int32, (16, LANES), 1)
    nothing = jnp.zeros((16, LANES), BF16)

    def coarse(index):
        return [
            spread[pl.ds(pl.multiple_of((part * per + 2 * index) * octants, 16), 16), :].astype(BF16)
            for part in range(parts)
        ]

    def chunk(c, carry):
        weight_copy(c).wait()
        phase_copy(c).wait()
        near, far = [], []
        for i in range(-1, CHUNK + 1):
            values = coarse(lax.rem(c * CHUNK + i + total, total))
            near.append([pltpu.roll(v, HW, 1) for v in values] if i < CHUNK else None)
            far.append([pltpu.roll(v, 64 + HW, 1) for v in values] if i >= 0 else None)
        for i in range(CHUNK):
            windows = (
                jnp.concatenate([jnp.where(lane_16 < HW, b, h) for b, h in zip(near[i], near[i + 1])], axis=0),
                jnp.concatenate([jnp.where(lane_16 < 64 + HW, h, a) for h, a in zip(far[i + 1], far[i + 2])], axis=0),
            )
            base = pl.multiple_of(c * span, span) + 4 * LANES * i
            real = [None] * 8
            imag = [None] * 8
            for half in range(2):
                high, low = [], []
                for tile in range(2):
                    at = pl.ds(base + (2 * half + tile) * LANES, LANES)
                    turned = jnp.take_along_axis(weights_in[:, at], turn, axis=0, mode="promise_in_bounds")
                    rest = turned - turned.astype(BF16).astype(F32)
                    high.append(jnp.concatenate([turned, turned], axis=0).astype(BF16))
                    low.append(jnp.concatenate([rest, rest], axis=0).astype(BF16))
                weights = [
                    jnp.concatenate(
                        [
                            jnp.concatenate([left * b for b in bands] + [nothing] * 5, axis=0),
                            jnp.concatenate([nothing] * 2 + [right * b for b in bands] + [nothing] * 3, axis=0),
                        ],
                        axis=1,
                    )
                    for left, right in (high, low)
                ]
                refined = jnp.dot(
                    jnp.concatenate([windows[half], windows[half]], axis=1),
                    jnp.concatenate(weights, axis=0),
                    preferred_element_type=F32,
                )
                for tile in range(2):
                    at = pl.ds(base + (2 * half + tile) * LANES, LANES)
                    sin_tile, cos_tile = sin_cos(phase_in[:, at])
                    for pol in range(2):
                        re = refined[8 * pol : 8 * pol + 8, tile * LANES : (tile + 1) * LANES]
                        im = refined[16 + 8 * pol : 24 + 8 * pol, tile * LANES : (tile + 1) * LANES]
                        spot = 2 * (2 * half + tile) + pol
                        real[spot] = re * cos_tile - im * sin_tile
                        imag[spot] = re * sin_tile + im * cos_tile
            pattern = jnp.concatenate([row_sums(real), row_sums(imag)], axis=0).astype(BF16)
            for g in range(groups):
                out_ref[g, c * CHUNK + i] = pattern
        return carry

    lax.fori_loop(0, chunks, chunk, 0)


def aggregate(children, present, interp, phase, groups):
    total = children.shape[0] // 32
    chunks = total // CHUNK
    anywhere = pl.BlockSpec(memory_space=pl.ANY)
    return pl.pallas_call(
        aggregate_kernel,
        in_specs=[anywhere, anywhere, anywhere, anywhere],
        out_specs=pl.BlockSpec(memory_space=pltpu.VMEM),
        out_shape=pltpu.VMEM((groups, total, 16, LANES), BF16),
        scratch_shapes=[
            pltpu.VMEM(children.shape, BF16),
            pltpu.VMEM(children.shape, F32),
            pltpu.VMEM(interp.shape, F32),
            pltpu.VMEM(phase.shape, F32),
            pltpu.SMEM(present.shape, jnp.int32),
            pltpu.SemaphoreType.DMA((16,)),
            pltpu.SemaphoreType.DMA,
            pltpu.SemaphoreType.DMA((chunks,)),
            pltpu.SemaphoreType.DMA((chunks,)),
        ],
        compiler_params=pltpu.CompilerParams(vmem_limit_bytes=LIMIT * 1024),
        name="aggregate",
    )(present, children, interp, phase)


def aggregate_local(children, present, interp, phase, groups=2):
    total = children.shape[5] // LANES
    rows = jnp.transpose(children.reshape(2, 8, 2, total, LANES), (0, 1, 3, 2, 4)).reshape(-1, LANES)
    return aggregate(rows, present, interp, phase, groups)


def translate_kernel(
    sources_ref, ids_ref, used_ref, pattern_ref, trans_ref, out_ref, places, table, unpacked, received, table_sem, out_sem
):
    slots, receivers = sources_ref.shape
    clusters = pattern_ref.shape[0] // 16
    batches = receivers // BATCH

    def out_copy(b):
        at = pl.ds(b * BATCH, BATCH)
        return pltpu.make_async_copy(received.at[:, at], out_ref.at[:, at], out_sem.at[b])

    slot_row = lax.broadcasted_iota(jnp.int32, (slots, receivers), 0)
    places[:slots, :] = jnp.where(slot_row < used_ref[...], sources_ref[...], clusters) * 16
    places[slots:, :] = ids_ref[...] * 8
    table_copy = pltpu.make_async_copy(places, table, table_sem)
    table_copy.start()

    def unpack(c, carry):
        at = pl.ds(pl.multiple_of(16 * c, 16), 16)
        unpacked[at, :] = pattern_ref[at, :].astype(F32)
        return carry

    lax.fori_loop(0, clusters, unpack, 0, unroll=8)
    unpacked[pl.ds(16 * clusters, 16), :] = jnp.zeros((16, LANES), F32)
    row = lax.broadcasted_iota(jnp.int32, (8, LANES), 0)
    even = (row & 1) == 0
    order = 2 * (row & 3) + (row >> 2)
    table_copy.wait()

    for receiver in range(receivers):
        real = imag = None
        for slot in range(slots):
            source = pl.multiple_of(table[slot, receiver], 16)
            operator = trans_ref[pl.ds(pl.multiple_of(table[slots + slot, receiver], 8), 8), :]
            re = unpacked[pl.ds(source, 8), :]
            im = unpacked[pl.ds(source + 8, 8), :]
            t_re = jnp.where(even, operator, pltpu.roll(operator, 1, 0))
            t_im = jnp.where(even, pltpu.roll(operator, 7, 0), operator)
            new_re = t_re * re - t_im * im
            new_im = t_re * im + t_im * re
            real = new_re if real is None else real + new_re
            imag = new_im if imag is None else imag + new_im
        received[0, receiver] = jnp.take_along_axis(real, order, axis=0, mode="promise_in_bounds")
        received[1, receiver] = jnp.take_along_axis(imag, order, axis=0, mode="promise_in_bounds")
        if (receiver + 1) % BATCH == 0:
            out_copy(receiver // BATCH).start()
    for b in range(batches):
        out_copy(b).wait()


def translate_local(sources, trans_ids, list_len, pattern, trans):
    kinds = trans.shape[1]
    receivers, slots = sources.shape
    clusters = pattern.shape[0]
    operators = jnp.transpose(
        jnp.transpose(trans, (1, 0, 2)).reshape(kinds, 2, 4, LANES), (0, 2, 1, 3)
    ).reshape(kinds * 8, LANES)
    inside = pl.BlockSpec(memory_space=pltpu.VMEM)
    out = pl.pallas_call(
        translate_kernel,
        in_specs=[inside] * 5,
        out_specs=pl.BlockSpec(memory_space=pl.ANY),
        out_shape=jax.ShapeDtypeStruct((2, receivers, 8, LANES), F32),
        scratch_shapes=[
            pltpu.VMEM((2 * slots, receivers), jnp.int32),
            pltpu.SMEM((2 * slots, receivers), jnp.int32),
            pltpu.VMEM((16 * (clusters + 1), LANES), F32),
            pltpu.VMEM((2, receivers, 8, LANES), F32),
            pltpu.SemaphoreType.DMA,
            pltpu.SemaphoreType.DMA((receivers // BATCH,)),
        ],
        compiler_params=pltpu.CompilerParams(vmem_limit_bytes=16 * 2**20),
        name="translate",
    )(sources.T, trans_ids.T, list_len.reshape(1, -1), pattern.reshape(-1, LANES), operators)
    return out.reshape(2, -1, 2, 1, 4 * LANES)


def local(children, present, interp, phase, trans, sources, trans_ids, list_len):
    pattern = aggregate_local(children, present, interp, phase, lax.axis_size("grp"))
    pattern = lax.all_to_all(
        pattern.reshape(-1, 16, LANES), ("grp", "ang"), 0, 0, tiled=True
    )
    return translate_local(sources, trans_ids, list_len, pattern, trans)


def solution(mesh):
    placed = (
        P(None, ("grp", "ang"), None, None, None, None),
        P(("grp", "ang"), None),
        P(),
        P(),
        P(None, None, "ang"),
        P("grp", None),
        P("grp", None),
        P("grp"),
    )
    return jax.shard_map(
        local,
        mesh=mesh,
        in_specs=placed,
        out_specs=P(None, "grp", None, None, "ang"),
        check_vma=False,
    )
```

```python
import functools

import jax
import jax.numpy as jnp
from jax import lax
from jax.experimental import pallas as pl
from jax.experimental.pallas import tpu as pltpu
from jax.sharding import PartitionSpec as P

HW = 4
LANES = 128
CHUNK = 32
LIMIT = 57000
BATCH = 8
F32 = jnp.float32
BF16 = jnp.bfloat16
ROOT = 2.0**0.5

SIN_TERMS = tuple(
    ROOT * v * 0.5 ** (2 * i + 1)
    for i, v in enumerate((1.0, -0.1666666567325592, 0.008333242498338223, -0.00019822783360723406, 2.634888232933008e-06))
)
COS_TERMS = tuple(
    ROOT * v * 0.25**i
    for i, v in enumerate(
        (1.0, -0.5, 0.0416666679084301, -0.0013888812391087413, 2.4786117137409747e-05, -2.6547101583673793e-07)
    )
)


def horner(terms, z):
    total = z * terms[-1] + terms[-2]
    for term in terms[-3::-1]:
        total = total * z + term
    return total


def sin_cos(angle):
    z = angle * angle
    sin_half = angle * horner(SIN_TERMS, z)
    cos_half = horner(COS_TERMS, z)
    return sin_half * cos_half, 1.0 - sin_half * sin_half


def row_sums(rows):
    place = lax.broadcasted_iota(jnp.int32, rows[0].shape, 0)
    for distance in (1, 2, 4):
        first = (place & distance) == 0
        rows = [
            jnp.where(first, a, b) + pltpu.roll(jnp.where(first, b, a), distance, 0)
            for a, b in zip(rows[0::2], rows[1::2])
        ]
    return rows[0]


def aggregate_kernel(
    present_ref, children_ref, interp_ref, phase_ref, out_ref,
    stored, spread, weights_in, phase_in, flags, child_sem, flag_sem, weight_sem, phase_sem,
):
    groups, total = out_ref.shape[:2]
    chunks = total // CHUNK
    span = 4 * LANES * CHUNK
    octants = 8
    parts = 2
    per = 2 * total

    def weight_copy(c):
        at = pl.ds(pl.multiple_of(c * span, span), span)
        return pltpu.make_async_copy(interp_ref.at[:, at], weights_in.at[:, at], weight_sem.at[c])

    def phase_copy(c):
        at = pl.ds(pl.multiple_of(c * span, span), span)
        return pltpu.make_async_copy(phase_ref.at[:, at], phase_in.at[:, at], phase_sem.at[c])

    def child_copy(k):
        at = pl.ds(k * per, per)
        return pltpu.make_async_copy(children_ref.at[at], stored.at[at], child_sem.at[k])

    flag_copy = pltpu.make_async_copy(present_ref, flags, flag_sem)
    flag_copy.start()
    for k in range(parts * octants):
        child_copy(k).start()
    for c in range(chunks):
        weight_copy(c).start()
        phase_copy(c).start()
    flag_copy.wait()

    for octant in range(octants):
        flag = flags[0, octant].astype(F32)
        for part in range(parts):
            child_copy(part * octants + octant).wait()

            def unpack(m, carry, flag=flag, octant=octant, part=part):
                at = pl.multiple_of((part * octants + octant) * per + 16 * m, 16)
                rows = stored[pl.ds(at, 16), :].astype(F32) * flag
                to = (part * per + 16 * m) * octants + octant
                spread[pl.ds(to, 8, stride=octants), :] = rows[:8]
                spread[pl.ds(to + 8 * octants, 8, stride=octants), :] = rows[8:]
                return carry

            lax.fori_loop(0, per // 16, unpack, 0, unroll=True)

    lane = lax.broadcasted_iota(jnp.int32, (8, LANES), 1)
    row = lax.broadcasted_iota(jnp.int32, (8, LANES), 0)
    turn = (row - lane // 4) & 7
    row16 = lax.broadcasted_iota(jnp.int32, (16, LANES), 0)
    lane16 = lax.broadcasted_iota(jnp.int32, (16, LANES), 1) // 4
    bands = []
    for i in range(3):
        tap = row16 + 16 * i - lane16
        bands.append(jnp.where((tap >= 0) & (tap < 8), 1.0, 0.0).astype(BF16))
    lane_16 = lax.broadcasted_iota(jnp.int32, (16, LANES), 1)
    nothing = jnp.zeros((16, LANES), BF16)

    def coarse(index):
        return [
            spread[pl.ds(pl.multiple_of((part * per + 2 * index) * octants, 16), 16), :].astype(BF16)
            for part in range(parts)
        ]

    def chunk(c, carry):
        weight_copy(c).wait()
        phase_copy(c).wait()
        near, far = [], []
        for i in range(-1, CHUNK + 1):
            values = coarse(lax.rem(c * CHUNK + i + total, total))
            near.append([pltpu.roll(v, HW, 1) for v in values] if i < CHUNK else None)
            far.append([pltpu.roll(v, 64 + HW, 1) for v in values] if i >= 0 else None)
        for i in range(CHUNK):
            windows = (
                jnp.concatenate([jnp.where(lane_16 < HW, b, h) for b, h in zip(near[i], near[i + 1])], axis=0),
                jnp.concatenate([jnp.where(lane_16 < 64 + HW, h, a) for h, a in zip(far[i + 1], far[i + 2])], axis=0),
            )
            base = pl.multiple_of(c * span, span) + 4 * LANES * i
            real = [None] * 8
            imag = [None] * 8
            for half in range(2):
                high, low = [], []
                for tile in range(2):
                    at = pl.ds(base + (2 * half + tile) * LANES, LANES)
                    turned = jnp.take_along_axis(weights_in[:, at], turn, axis=0, mode="promise_in_bounds")
                    rest = turned - turned.astype(BF16).astype(F32)
                    high.append(jnp.concatenate([turned, turned], axis=0).astype(BF16))
                    low.append(jnp.concatenate([rest, rest], axis=0).astype(BF16))
                weights = [
                    jnp.concatenate(
                        [
                            jnp.concatenate([left * b for b in bands] + [nothing] * 5, axis=0),
                            jnp.concatenate([nothing] * 2 + [right * b for b in bands] + [nothing] * 3, axis=0),
                        ],
                        axis=1,
                    )
                    for left, right in (high, low)
                ]
                refined = jnp.dot(
                    jnp.concatenate([windows[half], windows[half]], axis=1),
                    jnp.concatenate(weights, axis=0),
                    preferred_element_type=F32,
                )
                for tile in range(2):
                    at = pl.ds(base + (2 * half + tile) * LANES, LANES)
                    sin_tile, cos_tile = sin_cos(phase_in[:, at])
                    for pol in range(2):
                        re = refined[8 * pol : 8 * pol + 8, tile * LANES : (tile + 1) * LANES]
                        im = refined[16 + 8 * pol : 24 + 8 * pol, tile * LANES : (tile + 1) * LANES]
                        spot = 2 * (2 * half + tile) + pol
                        real[spot] = re * cos_tile - im * sin_tile
                        imag[spot] = re * sin_tile + im * cos_tile
            pattern = jnp.concatenate([row_sums(real), row_sums(imag)], axis=0).astype(BF16)
            for g in range(groups):
                out_ref[g, c * CHUNK + i] = pattern
        return carry

    lax.fori_loop(0, chunks, chunk, 0)


def aggregate(children, present, interp, phase, groups):
    total = children.shape[0] // 32
    chunks = total // CHUNK
    anywhere = pl.BlockSpec(memory_space=pl.ANY)
    return pl.pallas_call(
        aggregate_kernel,
        in_specs=[anywhere, anywhere, anywhere, anywhere],
        out_specs=pl.BlockSpec(memory_space=pltpu.VMEM),
        out_shape=pltpu.VMEM((groups, total, 16, LANES), BF16),
        scratch_shapes=[
            pltpu.VMEM(children.shape, BF16),
            pltpu.VMEM(children.shape, F32),
            pltpu.VMEM(interp.shape, F32),
            pltpu.VMEM(phase.shape, F32),
            pltpu.SMEM(present.shape, jnp.int32),
            pltpu.SemaphoreType.DMA((16,)),
            pltpu.SemaphoreType.DMA,
            pltpu.SemaphoreType.DMA((chunks,)),
            pltpu.SemaphoreType.DMA((chunks,)),
        ],
        compiler_params=pltpu.CompilerParams(vmem_limit_bytes=LIMIT * 1024),
        name="aggregate",
    )(present, children, interp, phase)


def aggregate_local(children, present, interp, phase, groups=2):
    total = children.shape[5] // LANES
    rows = jnp.transpose(children.reshape(2, 8, 2, total, LANES), (0, 1, 3, 2, 4)).reshape(-1, LANES)
    return aggregate(rows, present, interp, phase, groups)


def translate_kernel(
    sources_ref, ids_ref, used_ref, pattern_ref, trans_ref, out_ref, places, table, unpacked, spread_trans, received, table_sem, out_sem
):
    slots, receivers = sources_ref.shape
    clusters = pattern_ref.shape[0] // 16
    batches = receivers // BATCH

    def out_copy(b):
        at = pl.ds(b * BATCH, BATCH)
        return pltpu.make_async_copy(received.at[:, at], out_ref.at[:, at], out_sem.at[b])

    slot_row = lax.broadcasted_iota(jnp.int32, (slots, receivers), 0)
    places[:slots, :] = jnp.where(slot_row < used_ref[...], sources_ref[...], clusters) * 16
    places[slots:, :] = ids_ref[...] * 16
    table_copy = pltpu.make_async_copy(places, table, table_sem)
    table_copy.start()

    def unpack(c, carry):
        at = pl.ds(pl.multiple_of(16 * c, 16), 16)
        unpacked[at, :] = pattern_ref[at, :].astype(F32)
        return carry

    lax.fori_loop(0, clusters, unpack, 0, unroll=8)
    unpacked[pl.ds(16 * clusters, 16), :] = jnp.zeros((16, LANES), F32)
    row = lax.broadcasted_iota(jnp.int32, (8, LANES), 0)
    even = (row & 1) == 0
    order = 2 * (row & 3) + (row >> 2)

    def expand(k, carry):
        operator = trans_ref[pl.ds(pl.multiple_of(8 * k, 8), 8), :]
        at = pl.multiple_of(16 * k, 16)
        spread_trans[pl.ds(at, 8), :] = jnp.where(even, operator, pltpu.roll(operator, 1, 0))
        spread_trans[pl.ds(at + 8, 8), :] = jnp.where(even, pltpu.roll(operator, 7, 0), operator)
        return carry

    lax.fori_loop(0, trans_ref.shape[0] // 8, expand, 0, unroll=4)
    table_copy.wait()

    for receiver in range(receivers):
        real = imag = None
        for slot in range(slots):
            source = pl.multiple_of(table[slot, receiver], 16)
            operator = pl.multiple_of(table[slots + slot, receiver], 16)
            re = unpacked[pl.ds(source, 8), :]
            im = unpacked[pl.ds(source + 8, 8), :]
            t_re = spread_trans[pl.ds(operator, 8), :]
            t_im = spread_trans[pl.ds(operator + 8, 8), :]
            new_re = t_re * re - t_im * im
            new_im = t_re * im + t_im * re
            real = new_re if real is None else real + new_re
            imag = new_im if imag is None else imag + new_im
        received[0, receiver] = jnp.take_along_axis(real, order, axis=0, mode="promise_in_bounds")
        received[1, receiver] = jnp.take_along_axis(imag, order, axis=0, mode="promise_in_bounds")
        if (receiver + 1) % BATCH == 0:
            out_copy(receiver // BATCH).start()
    for b in range(batches):
        out_copy(b).wait()


def translate_local(sources, trans_ids, list_len, pattern, trans):
    kinds = trans.shape[1]
    receivers, slots = sources.shape
    clusters = pattern.shape[0]
    operators = jnp.transpose(
        jnp.transpose(trans, (1, 0, 2)).reshape(kinds, 2, 4, LANES), (0, 2, 1, 3)
    ).reshape(kinds * 8, LANES)
    inside = pl.BlockSpec(memory_space=pltpu.VMEM)
    out = pl.pallas_call(
        translate_kernel,
        in_specs=[inside] * 5,
        out_specs=pl.BlockSpec(memory_space=pl.ANY),
        out_shape=jax.ShapeDtypeStruct((2, receivers, 8, LANES), F32),
        scratch_shapes=[
            pltpu.VMEM((2 * slots, receivers), jnp.int32),
            pltpu.SMEM((2 * slots, receivers), jnp.int32),
            pltpu.VMEM((16 * (clusters + 1), LANES), F32),
            pltpu.VMEM((16 * kinds, LANES), F32),
            pltpu.VMEM((2, receivers, 8, LANES), F32),
            pltpu.SemaphoreType.DMA,
            pltpu.SemaphoreType.DMA((receivers // BATCH,)),
        ],
        compiler_params=pltpu.CompilerParams(vmem_limit_bytes=16 * 2**20),
        name="translate",
    )(sources.T, trans_ids.T, list_len.reshape(1, -1), pattern.reshape(-1, LANES), operators)
    return out.reshape(2, -1, 2, 1, 4 * LANES)


def local(children, present, interp, phase, trans, sources, trans_ids, list_len):
    pattern = aggregate_local(children, present, interp, phase, lax.axis_size("grp"))
    pattern = lax.all_to_all(
        pattern.reshape(-1, 16, LANES), ("grp", "ang"), 0, 0, tiled=True
    )
    return translate_local(sources, trans_ids, list_len, pattern, trans)


def solution(mesh):
    placed = (
        P(None, ("grp", "ang"), None, None, None, None),
        P(("grp", "ang"), None),
        P(),
        P(),
        P(None, None, "ang"),
        P("grp", None),
        P("grp", None),
        P("grp"),
    )
    return jax.shard_map(
        local,
        mesh=mesh,
        in_specs=placed,
        out_specs=P(None, "grp", None, None, "ang"),
        check_vma=False,
    )
```

```python
import functools

import jax
import jax.numpy as jnp
from jax import lax
from jax.experimental import pallas as pl
from jax.experimental.pallas import tpu as pltpu
from jax.sharding import PartitionSpec as P

HW = 4
LANES = 128
CHUNK = 32
AGAIN = 72
LIMIT = 57000
BATCH = 8
F32 = jnp.float32
BF16 = jnp.bfloat16
ROOT = 2.0**0.5

SIN_TERMS = tuple(
    ROOT * v * 0.5 ** (2 * i + 1)
    for i, v in enumerate((1.0, -0.1666666567325592, 0.008333242498338223, -0.00019822783360723406, 2.634888232933008e-06))
)
COS_TERMS = tuple(
    ROOT * v * 0.25**i
    for i, v in enumerate(
        (1.0, -0.5, 0.0416666679084301, -0.0013888812391087413, 2.4786117137409747e-05, -2.6547101583673793e-07)
    )
)


def horner(terms, z):
    total = z * terms[-1] + terms[-2]
    for term in terms[-3::-1]:
        total = total * z + term
    return total


def sin_cos(angle):
    z = angle * angle
    sin_half = angle * horner(SIN_TERMS, z)
    cos_half = horner(COS_TERMS, z)
    return sin_half * cos_half, 1.0 - sin_half * sin_half


def row_sums(rows):
    place = lax.broadcasted_iota(jnp.int32, rows[0].shape, 0)
    for distance in (1, 2, 4):
        first = (place & distance) == 0
        rows = [
            jnp.where(first, a, b) + pltpu.roll(jnp.where(first, b, a), distance, 0)
            for a, b in zip(rows[0::2], rows[1::2])
        ]
    return rows[0]


def aggregate_kernel(
    present_ref, children_ref, interp_ref, phase_ref, out_ref,
    stored, spread, weights_in, phase_in, flags, child_sem, flag_sem, weight_sem, phase_sem,
):
    groups, total = out_ref.shape[:2]
    chunks = total // CHUNK
    span = 4 * LANES * CHUNK
    octants = 8
    parts = 2
    per = 2 * total

    def weight_copy(c):
        at = pl.ds(pl.multiple_of(c * span, span), span)
        return pltpu.make_async_copy(interp_ref.at[:, at], weights_in.at[:, at], weight_sem.at[c])

    def phase_copy(c):
        at = pl.ds(pl.multiple_of(c * span, span), span)
        return pltpu.make_async_copy(phase_ref.at[:, at], phase_in.at[:, at], phase_sem.at[c])

    def child_copy(k):
        at = pl.ds(k * per, per)
        return pltpu.make_async_copy(children_ref.at[at], stored.at[at], child_sem.at[k])

    flag_copy = pltpu.make_async_copy(present_ref, flags, flag_sem)
    flag_copy.start()
    for k in range(parts * octants):
        child_copy(k).start()
    for c in range(chunks):
        weight_copy(c).start()
        phase_copy(c).start()
    flag_copy.wait()

    for octant in range(octants):
        flag = flags[0, octant].astype(F32)
        for part in range(parts):
            child_copy(part * octants + octant).wait()

            def unpack(m, carry, flag=flag, octant=octant, part=part):
                at = pl.multiple_of((part * octants + octant) * per + 16 * m, 16)
                rows = stored[pl.ds(at, 16), :].astype(F32) * flag
                to = (part * per + 16 * m) * octants + octant
                spread[pl.ds(to, 8, stride=octants), :] = rows[:8]
                spread[pl.ds(to + 8 * octants, 8, stride=octants), :] = rows[8:]
                return carry

            lax.fori_loop(0, per // 16, unpack, 0, unroll=True)

    lane = lax.broadcasted_iota(jnp.int32, (8, LANES), 1)
    row = lax.broadcasted_iota(jnp.int32, (8, LANES), 0)
    turn = (row - lane // 4) & 7
    row16 = lax.broadcasted_iota(jnp.int32, (16, LANES), 0)
    lane16 = lax.broadcasted_iota(jnp.int32, (16, LANES), 1) // 4
    def bands(first):
        taps = [row16 + 16 * i - first - lane16 for i in range(3)]
        return [jnp.where((tap >= 0) & (tap < 8), 1.0, 0.0).astype(BF16) for tap in taps]

    high_bands, low_bands = bands(0), bands(8)
    lane_16 = lax.broadcasted_iota(jnp.int32, (16, LANES), 1)
    nothing = jnp.zeros((16, LANES), BF16)

    shifts = (HW, HW + AGAIN, LANES // 2 + HW, LANES // 2 + HW + AGAIN - LANES)

    def shifted(index):
        tiles = [
            spread[pl.ds(pl.multiple_of((part * per + 2 * index) * octants, 16), 16), :].astype(BF16)
            for part in range(parts)
        ]
        return [[pltpu.roll(t, shift, 1) for shift in shifts] for t in tiles]

    def windows_of(before, now, after):
        first, second = [], []
        for part in range(parts):
            near, near_again, far, far_again = now[part]
            left = jnp.where(
                lane_16 < HW,
                before[part][0],
                jnp.where(lane_16 < AGAIN, near, jnp.where(lane_16 < AGAIN + HW, before[part][1], near_again)),
            )
            first.append(jnp.concatenate([left, near_again], axis=1))
            left = jnp.where(lane_16 < shifts[2], far, jnp.where(lane_16 < AGAIN, after[part][2], far_again))
            right = jnp.where(lane_16 < shifts[3], far_again, after[part][3])
            second.append(jnp.concatenate([left, right], axis=1))
        return jnp.concatenate(first, axis=0), jnp.concatenate(second, axis=0)

    def chunk(c, carry):
        weight_copy(c).wait()
        phase_copy(c).wait()
        moved = [shifted(lax.rem(c * CHUNK + i + total, total)) for i in range(-1, CHUNK + 1)]
        for i in range(CHUNK):
            windows = windows_of(*moved[i : i + 3])
            base = pl.multiple_of(c * span, span) + 4 * LANES * i
            real = [None] * 8
            imag = [None] * 8
            for half in range(2):
                high, low = [], []
                for tile in range(2):
                    at = pl.ds(base + (2 * half + tile) * LANES, LANES)
                    turned = jnp.take_along_axis(weights_in[:, at], turn, axis=0, mode="promise_in_bounds")
                    rest = turned - turned.astype(BF16).astype(F32)
                    high.append(jnp.concatenate([turned, turned], axis=0).astype(BF16))
                    low.append(jnp.concatenate([rest, rest], axis=0).astype(BF16))
                left, right = ([part * b for b in high_bands] for part in high)
                left_low, right_low = ([part * b for b in low_bands] for part in low)
                weights = jnp.concatenate(
                    [
                        jnp.concatenate(left + [nothing] + left_low + [nothing] * 9, axis=0),
                        jnp.concatenate([nothing] * 2 + right + [nothing] + right_low + [nothing] * 7, axis=0),
                    ],
                    axis=1,
                )
                refined = jnp.dot(
                    windows[half],
                    weights,
                    preferred_element_type=F32,
                )
                for tile in range(2):
                    at = pl.ds(base + (2 * half + tile) * LANES, LANES)
                    sin_tile, cos_tile = sin_cos(phase_in[:, at])
                    for pol in range(2):
                        re = refined[8 * pol : 8 * pol + 8, tile * LANES : (tile + 1) * LANES]
                        im = refined[16 + 8 * pol : 24 + 8 * pol, tile * LANES : (tile + 1) * LANES]
                        spot = 2 * (2 * half + tile) + pol
                        real[spot] = re * cos_tile - im * sin_tile
                        imag[spot] = re * sin_tile + im * cos_tile
            pattern = jnp.concatenate([row_sums(real), row_sums(imag)], axis=0).astype(BF16)
            for g in range(groups):
                out_ref[g, c * CHUNK + i] = pattern
        return carry

    lax.fori_loop(0, chunks, chunk, 0)


def aggregate(children, present, interp, phase, groups):
    total = children.shape[0] // 32
    chunks = total // CHUNK
    anywhere = pl.BlockSpec(memory_space=pl.ANY)
    return pl.pallas_call(
        aggregate_kernel,
        in_specs=[anywhere, anywhere, anywhere, anywhere],
        out_specs=pl.BlockSpec(memory_space=pltpu.VMEM),
        out_shape=pltpu.VMEM((groups, total, 16, LANES), BF16),
        scratch_shapes=[
            pltpu.VMEM(children.shape, BF16),
            pltpu.VMEM(children.shape, F32),
            pltpu.VMEM(interp.shape, F32),
            pltpu.VMEM(phase.shape, F32),
            pltpu.SMEM(present.shape, jnp.int32),
            pltpu.SemaphoreType.DMA((16,)),
            pltpu.SemaphoreType.DMA,
            pltpu.SemaphoreType.DMA((chunks,)),
            pltpu.SemaphoreType.DMA((chunks,)),
        ],
        compiler_params=pltpu.CompilerParams(vmem_limit_bytes=LIMIT * 1024),
        name="aggregate",
    )(present, children, interp, phase)


def aggregate_local(children, present, interp, phase, groups=2):
    total = children.shape[5] // LANES
    rows = jnp.transpose(children.reshape(2, 8, 2, total, LANES), (0, 1, 3, 2, 4)).reshape(-1, LANES)
    return aggregate(rows, present, interp, phase, groups)


def translate_kernel(
    sources_ref, ids_ref, used_ref, pattern_ref, trans_ref, out_ref, places, table, unpacked, spread_trans, received, table_sem, out_sem
):
    slots, receivers = sources_ref.shape
    clusters = pattern_ref.shape[0] // 16
    batches = receivers // BATCH

    def out_copy(b):
        at = pl.ds(b * BATCH, BATCH)
        return pltpu.make_async_copy(received.at[:, at], out_ref.at[:, at], out_sem.at[b])

    slot_row = lax.broadcasted_iota(jnp.int32, (slots, receivers), 0)
    places[:slots, :] = jnp.where(slot_row < used_ref[...], sources_ref[...], clusters) * 16
    places[slots:, :] = ids_ref[...] * 16
    table_copy = pltpu.make_async_copy(places, table, table_sem)
    table_copy.start()

    def unpack(c, carry):
        at = pl.ds(pl.multiple_of(16 * c, 16), 16)
        unpacked[at, :] = pattern_ref[at, :].astype(F32)
        return carry

    lax.fori_loop(0, clusters, unpack, 0, unroll=8)
    unpacked[pl.ds(16 * clusters, 16), :] = jnp.zeros((16, LANES), F32)
    row = lax.broadcasted_iota(jnp.int32, (8, LANES), 0)
    even = (row & 1) == 0
    order = 2 * (row & 3) + (row >> 2)

    def expand(k, carry):
        operator = trans_ref[pl.ds(pl.multiple_of(8 * k, 8), 8), :]
        at = pl.multiple_of(16 * k, 16)
        spread_trans[pl.ds(at, 8), :] = jnp.where(even, operator, pltpu.roll(operator, 1, 0))
        spread_trans[pl.ds(at + 8, 8), :] = jnp.where(even, pltpu.roll(operator, 7, 0), operator)
        return carry

    lax.fori_loop(0, trans_ref.shape[0] // 8, expand, 0, unroll=4)
    table_copy.wait()

    for receiver in range(receivers):
        real = imag = None
        for slot in range(slots):
            source = pl.multiple_of(table[slot, receiver], 16)
            operator = pl.multiple_of(table[slots + slot, receiver], 16)
            re = unpacked[pl.ds(source, 8), :]
            im = unpacked[pl.ds(source + 8, 8), :]
            t_re = spread_trans[pl.ds(operator, 8), :]
            t_im = spread_trans[pl.ds(operator + 8, 8), :]
            new_re = t_re * re - t_im * im
            new_im = t_re * im + t_im * re
            real = new_re if real is None else real + new_re
            imag = new_im if imag is None else imag + new_im
        received[0, receiver] = jnp.take_along_axis(real, order, axis=0, mode="promise_in_bounds")
        received[1, receiver] = jnp.take_along_axis(imag, order, axis=0, mode="promise_in_bounds")
        if (receiver + 1) % BATCH == 0:
            out_copy(receiver // BATCH).start()
    for b in range(batches):
        out_copy(b).wait()


def translate_local(sources, trans_ids, list_len, pattern, trans):
    kinds = trans.shape[1]
    receivers, slots = sources.shape
    clusters = pattern.shape[0]
    operators = jnp.transpose(
        jnp.transpose(trans, (1, 0, 2)).reshape(kinds, 2, 4, LANES), (0, 2, 1, 3)
    ).reshape(kinds * 8, LANES)
    inside = pl.BlockSpec(memory_space=pltpu.VMEM)
    out = pl.pallas_call(
        translate_kernel,
        in_specs=[inside] * 5,
        out_specs=pl.BlockSpec(memory_space=pl.ANY),
        out_shape=jax.ShapeDtypeStruct((2, receivers, 8, LANES), F32),
        scratch_shapes=[
            pltpu.VMEM((2 * slots, receivers), jnp.int32),
            pltpu.SMEM((2 * slots, receivers), jnp.int32),
            pltpu.VMEM((16 * (clusters + 1), LANES), F32),
            pltpu.VMEM((16 * kinds, LANES), F32),
            pltpu.VMEM((2, receivers, 8, LANES), F32),
            pltpu.SemaphoreType.DMA,
            pltpu.SemaphoreType.DMA((receivers // BATCH,)),
        ],
        compiler_params=pltpu.CompilerParams(vmem_limit_bytes=16 * 2**20),
        name="translate",
    )(sources.T, trans_ids.T, list_len.reshape(1, -1), pattern.reshape(-1, LANES), operators)
    return out.reshape(2, -1, 2, 1, 4 * LANES)


def local(children, present, interp, phase, trans, sources, trans_ids, list_len):
    pattern = aggregate_local(children, present, interp, phase, lax.axis_size("grp"))
    pattern = lax.all_to_all(
        pattern.reshape(-1, 16, LANES), ("grp", "ang"), 0, 0, tiled=True
    )
    return translate_local(sources, trans_ids, list_len, pattern, trans)


def solution(mesh):
    placed = (
        P(None, ("grp", "ang"), None, None, None, None),
        P(("grp", "ang"), None),
        P(),
        P(),
        P(None, None, "ang"),
        P("grp", None),
        P("grp", None),
        P("grp"),
    )
    return jax.shard_map(
        local,
        mesh=mesh,
        in_specs=placed,
        out_specs=P(None, "grp", None, None, "ang"),
        check_vma=False,
    )
```

```python
import functools

import jax
import jax.numpy as jnp
from jax import lax
from jax.experimental import pallas as pl
from jax.experimental.pallas import tpu as pltpu
from jax.sharding import PartitionSpec as P

HW = 4
LANES = 128
CHUNK = 32
AGAIN = 72
LIMIT = 57000
BATCH = 8
F32 = jnp.float32
BF16 = jnp.bfloat16
ROOT = 2.0**0.5

SIN_TERMS = tuple(
    ROOT * v * 0.5 ** (2 * i + 1)
    for i, v in enumerate((1.0, -0.1666666567325592, 0.008333242498338223, -0.00019822783360723406, 2.634888232933008e-06))
)
COS_TERMS = tuple(
    ROOT * v * 0.25**i
    for i, v in enumerate(
        (1.0, -0.5, 0.0416666679084301, -0.0013888812391087413, 2.4786117137409747e-05, -2.6547101583673793e-07)
    )
)


def horner(terms, z):
    total = z * terms[-1] + terms[-2]
    for term in terms[-3::-1]:
        total = total * z + term
    return total


def sin_cos(angle):
    z = angle * angle
    sin_half = angle * horner(SIN_TERMS, z)
    cos_half = horner(COS_TERMS, z)
    return sin_half * cos_half, 1.0 - sin_half * sin_half


def row_sums(rows):
    place = lax.broadcasted_iota(jnp.int32, rows[0].shape, 0)
    for distance in (1, 2, 4):
        first = (place & distance) == 0
        rows = [
            jnp.where(first, a, b) + pltpu.roll(jnp.where(first, b, a), distance, 0)
            for a, b in zip(rows[0::2], rows[1::2])
        ]
    return rows[0]


def aggregate_kernel(
    present_ref, children_ref, interp_ref, phase_ref, out_ref,
    stored, spread, weights_in, phase_in, flags, child_sem, flag_sem, weight_sem, phase_sem,
):
    groups, total = out_ref.shape[:2]
    chunks = total // CHUNK
    span = 4 * LANES * CHUNK
    octants = 8
    parts = 2
    per = 2 * total

    def weight_copy(c):
        at = pl.ds(pl.multiple_of(c * span, span), span)
        return pltpu.make_async_copy(interp_ref.at[:, at], weights_in.at[:, at], weight_sem.at[c])

    def phase_copy(c):
        at = pl.ds(pl.multiple_of(c * span, span), span)
        return pltpu.make_async_copy(phase_ref.at[:, at], phase_in.at[:, at], phase_sem.at[c])

    def child_copy(k):
        at = pl.ds(k * per, per)
        return pltpu.make_async_copy(children_ref.at[at], stored.at[at], child_sem.at[k])

    flag_copy = pltpu.make_async_copy(present_ref, flags, flag_sem)
    flag_copy.start()
    for k in range(parts * octants):
        child_copy(k).start()
    for c in range(chunks):
        weight_copy(c).start()
        phase_copy(c).start()
    flag_copy.wait()

    for octant in range(octants):
        flag = flags[0, octant].astype(F32)
        for part in range(parts):
            child_copy(part * octants + octant).wait()

            def unpack(m, carry, flag=flag, octant=octant, part=part):
                at = pl.multiple_of((part * octants + octant) * per + 16 * m, 16)
                rows = stored[pl.ds(at, 16), :].astype(F32) * flag
                to = (part * per + 16 * m) * octants + octant
                spread[pl.ds(to, 8, stride=octants), :] = rows[:8]
                spread[pl.ds(to + 8 * octants, 8, stride=octants), :] = rows[8:]
                return carry

            lax.fori_loop(0, per // 16, unpack, 0, unroll=True)

    lane = lax.broadcasted_iota(jnp.int32, (8, LANES), 1)
    row = lax.broadcasted_iota(jnp.int32, (8, LANES), 0)
    turn = (row - lane // 4) & 7
    row16 = lax.broadcasted_iota(jnp.int32, (16, LANES), 0)
    lane16 = lax.broadcasted_iota(jnp.int32, (16, LANES), 1) // 4
    def bands(first):
        taps = [row16 + 16 * i - first - lane16 for i in range(3)]
        return [jnp.where((tap >= 0) & (tap < 8), 1.0, 0.0).astype(BF16) for tap in taps]

    high_bands, low_bands = bands(0), bands(8)
    lane_16 = lax.broadcasted_iota(jnp.int32, (16, LANES), 1)
    nothing = jnp.zeros((16, LANES), BF16)

    shifts = (HW, HW + AGAIN, LANES // 2 + HW, LANES // 2 + HW + AGAIN - LANES)

    def shifted(index):
        tiles = [
            spread[pl.ds(pl.multiple_of((part * per + 2 * index) * octants, 16), 16), :].astype(BF16)
            for part in range(parts)
        ]
        moved = []
        for tile in tiles:
            near, near_again, far, far_again = (pltpu.roll(tile, shift, 1) for shift in shifts)
            once = lane_16 < AGAIN
            moved.append((jnp.where(once, near, near_again), near_again, jnp.where(once, far, far_again), far_again))
        return moved

    from_before = (lane_16 < HW) | ((lane_16 >= AGAIN) & (lane_16 < AGAIN + HW))
    from_after = (lane_16 >= shifts[2]) & (lane_16 < AGAIN)

    def windows_of(before, now, after):
        first, second = [], []
        for part in range(parts):
            near, near_again, far, far_again = now[part]
            first.append(jnp.concatenate([jnp.where(from_before, before[part][0], near), near_again], axis=1))
            left = jnp.where(from_after, after[part][2], far)
            right = jnp.where(lane_16 < shifts[3], far_again, after[part][3])
            second.append(jnp.concatenate([left, right], axis=1))
        return jnp.concatenate(first, axis=0), jnp.concatenate(second, axis=0)

    def chunk(c, carry):
        weight_copy(c).wait()
        phase_copy(c).wait()
        moved = [shifted(lax.rem(c * CHUNK + i + total, total)) for i in range(-1, CHUNK + 1)]
        for i in range(CHUNK):
            windows = windows_of(*moved[i : i + 3])
            base = pl.multiple_of(c * span, span) + 4 * LANES * i
            real = [None] * 8
            imag = [None] * 8
            for half in range(2):
                high, low = [], []
                for tile in range(2):
                    at = pl.ds(base + (2 * half + tile) * LANES, LANES)
                    turned = jnp.take_along_axis(weights_in[:, at], turn, axis=0, mode="promise_in_bounds")
                    rest = turned - turned.astype(BF16).astype(F32)
                    high.append(jnp.concatenate([turned, turned], axis=0).astype(BF16))
                    low.append(jnp.concatenate([rest, rest], axis=0).astype(BF16))
                left, right = ([part * b for b in high_bands] for part in high)
                left_low, right_low = ([part * b for b in low_bands] for part in low)
                weights = jnp.concatenate(
                    [
                        jnp.concatenate(left + [nothing] + left_low + [nothing] * 9, axis=0),
                        jnp.concatenate([nothing] * 2 + right + [nothing] + right_low + [nothing] * 7, axis=0),
                    ],
                    axis=1,
                )
                refined = jnp.dot(
                    windows[half],
                    weights,
                    preferred_element_type=F32,
                )
                for tile in range(2):
                    at = pl.ds(base + (2 * half + tile) * LANES, LANES)
                    sin_tile, cos_tile = sin_cos(phase_in[:, at])
                    for pol in range(2):
                        re = refined[8 * pol : 8 * pol + 8, tile * LANES : (tile + 1) * LANES]
                        im = refined[16 + 8 * pol : 24 + 8 * pol, tile * LANES : (tile + 1) * LANES]
                        spot = 2 * (2 * half + tile) + pol
                        real[spot] = re * cos_tile - im * sin_tile
                        imag[spot] = re * sin_tile + im * cos_tile
            pattern = jnp.concatenate([row_sums(real), row_sums(imag)], axis=0).astype(BF16)
            for g in range(groups):
                out_ref[g, c * CHUNK + i] = pattern
        return carry

    lax.fori_loop(0, chunks, chunk, 0)


def aggregate(children, present, interp, phase, groups):
    total = children.shape[0] // 32
    chunks = total // CHUNK
    anywhere = pl.BlockSpec(memory_space=pl.ANY)
    return pl.pallas_call(
        aggregate_kernel,
        in_specs=[anywhere, anywhere, anywhere, anywhere],
        out_specs=pl.BlockSpec(memory_space=pltpu.VMEM),
        out_shape=pltpu.VMEM((groups, total, 16, LANES), BF16),
        scratch_shapes=[
            pltpu.VMEM(children.shape, BF16),
            pltpu.VMEM(children.shape, F32),
            pltpu.VMEM(interp.shape, F32),
            pltpu.VMEM(phase.shape, F32),
            pltpu.SMEM(present.shape, jnp.int32),
            pltpu.SemaphoreType.DMA((16,)),
            pltpu.SemaphoreType.DMA,
            pltpu.SemaphoreType.DMA((chunks,)),
            pltpu.SemaphoreType.DMA((chunks,)),
        ],
        compiler_params=pltpu.CompilerParams(vmem_limit_bytes=LIMIT * 1024),
        name="aggregate",
    )(present, children, interp, phase)


def aggregate_local(children, present, interp, phase, groups=2):
    total = children.shape[5] // LANES
    rows = jnp.transpose(children.reshape(2, 8, 2, total, LANES), (0, 1, 3, 2, 4)).reshape(-1, LANES)
    return aggregate(rows, present, interp, phase, groups)


def translate_kernel(
    sources_ref, ids_ref, used_ref, pattern_ref, trans_ref, out_ref, places, table, unpacked, spread_trans, received, table_sem, out_sem
):
    slots, receivers = sources_ref.shape
    clusters = pattern_ref.shape[0] // 16
    batches = receivers // BATCH

    def out_copy(b):
        at = pl.ds(b * BATCH, BATCH)
        return pltpu.make_async_copy(received.at[:, at], out_ref.at[:, at], out_sem.at[b])

    slot_row = lax.broadcasted_iota(jnp.int32, (slots, receivers), 0)
    places[:slots, :] = jnp.where(slot_row < used_ref[...], sources_ref[...], clusters) * 16
    places[slots:, :] = ids_ref[...] * 16
    table_copy = pltpu.make_async_copy(places, table, table_sem)
    table_copy.start()

    def unpack(c, carry):
        at = pl.ds(pl.multiple_of(16 * c, 16), 16)
        unpacked[at, :] = pattern_ref[at, :].astype(F32)
        return carry

    lax.fori_loop(0, clusters, unpack, 0, unroll=8)
    unpacked[pl.ds(16 * clusters, 16), :] = jnp.zeros((16, LANES), F32)
    row = lax.broadcasted_iota(jnp.int32, (8, LANES), 0)
    even = (row & 1) == 0
    order = 2 * (row & 3) + (row >> 2)

    def expand(k, carry):
        operator = trans_ref[pl.ds(pl.multiple_of(8 * k, 8), 8), :]
        at = pl.multiple_of(16 * k, 16)
        spread_trans[pl.ds(at, 8), :] = jnp.where(even, operator, pltpu.roll(operator, 1, 0))
        spread_trans[pl.ds(at + 8, 8), :] = jnp.where(even, pltpu.roll(operator, 7, 0), operator)
        return carry

    lax.fori_loop(0, trans_ref.shape[0] // 8, expand, 0, unroll=4)
    table_copy.wait()

    for receiver in range(receivers):
        real = imag = None
        for slot in range(slots):
            source = pl.multiple_of(table[slot, receiver], 16)
            operator = pl.multiple_of(table[slots + slot, receiver], 16)
            re = unpacked[pl.ds(source, 8), :]
            im = unpacked[pl.ds(source + 8, 8), :]
            t_re = spread_trans[pl.ds(operator, 8), :]
            t_im = spread_trans[pl.ds(operator + 8, 8), :]
            new_re = t_re * re - t_im * im
            new_im = t_re * im + t_im * re
            real = new_re if real is None else real + new_re
            imag = new_im if imag is None else imag + new_im
        received[0, receiver] = jnp.take_along_axis(real, order, axis=0, mode="promise_in_bounds")
        received[1, receiver] = jnp.take_along_axis(imag, order, axis=0, mode="promise_in_bounds")
        if (receiver + 1) % BATCH == 0:
            out_copy(receiver // BATCH).start()
    for b in range(batches):
        out_copy(b).wait()


def translate_local(sources, trans_ids, list_len, pattern, trans):
    kinds = trans.shape[1]
    receivers, slots = sources.shape
    clusters = pattern.shape[0]
    operators = jnp.transpose(
        jnp.transpose(trans, (1, 0, 2)).reshape(kinds, 2, 4, LANES), (0, 2, 1, 3)
    ).reshape(kinds * 8, LANES)
    inside = pl.BlockSpec(memory_space=pltpu.VMEM)
    out = pl.pallas_call(
        translate_kernel,
        in_specs=[inside] * 5,
        out_specs=pl.BlockSpec(memory_space=pl.ANY),
        out_shape=jax.ShapeDtypeStruct((2, receivers, 8, LANES), F32),
        scratch_shapes=[
            pltpu.VMEM((2 * slots, receivers), jnp.int32),
            pltpu.SMEM((2 * slots, receivers), jnp.int32),
            pltpu.VMEM((16 * (clusters + 1), LANES), F32),
            pltpu.VMEM((16 * kinds, LANES), F32),
            pltpu.VMEM((2, receivers, 8, LANES), F32),
            pltpu.SemaphoreType.DMA,
            pltpu.SemaphoreType.DMA((receivers // BATCH,)),
        ],
        compiler_params=pltpu.CompilerParams(vmem_limit_bytes=16 * 2**20),
        name="translate",
    )(sources.T, trans_ids.T, list_len.reshape(1, -1), pattern.reshape(-1, LANES), operators)
    return out.reshape(2, -1, 2, 1, 4 * LANES)


def local(children, present, interp, phase, trans, sources, trans_ids, list_len):
    pattern = aggregate_local(children, present, interp, phase, lax.axis_size("grp"))
    pattern = lax.all_to_all(
        pattern.reshape(-1, 16, LANES), ("grp", "ang"), 0, 0, tiled=True
    )
    return translate_local(sources, trans_ids, list_len, pattern, trans)


def solution(mesh):
    placed = (
        P(None, ("grp", "ang"), None, None, None, None),
        P(("grp", "ang"), None),
        P(),
        P(),
        P(None, None, "ang"),
        P("grp", None),
        P("grp", None),
        P("grp"),
    )
    return jax.shard_map(
        local,
        mesh=mesh,
        in_specs=placed,
        out_specs=P(None, "grp", None, None, "ang"),
        check_vma=False,
    )
```

```python
import functools

import jax
import jax.numpy as jnp
from jax import lax
from jax.experimental import pallas as pl
from jax.experimental.pallas import tpu as pltpu
from jax.sharding import PartitionSpec as P

HW = 4
LANES = 128
CHUNK = 32
AGAIN = 72
LIMIT = 57000
BATCH = 8
F32 = jnp.float32
BF16 = jnp.bfloat16
ROOT = 2.0**0.5

SIN_TERMS = tuple(
    ROOT * v * 0.5 ** (2 * i + 1)
    for i, v in enumerate((1.0, -0.1666666567325592, 0.008333242498338223, -0.00019822783360723406, 2.634888232933008e-06))
)
COS_TERMS = tuple(
    ROOT * v * 0.25**i
    for i, v in enumerate(
        (1.0, -0.5, 0.0416666679084301, -0.0013888812391087413, 2.4786117137409747e-05, -2.6547101583673793e-07)
    )
)


def horner(terms, z):
    total = z * terms[-1] + terms[-2]
    for term in terms[-3::-1]:
        total = total * z + term
    return total


def sin_cos(angle):
    z = angle * angle
    sin_half = angle * horner(SIN_TERMS, z)
    cos_half = horner(COS_TERMS, z)
    return sin_half * cos_half, 1.0 - sin_half * sin_half


def row_sums(rows):
    place = lax.broadcasted_iota(jnp.int32, rows[0].shape, 0)
    rows = [a + pltpu.roll(b, 1, 0) for a, b in zip(rows[0::2], rows[1::2])]
    for distance in (2, 4):
        first = (place & distance) == 0
        rows = [
            jnp.where(first, a, b) + pltpu.roll(jnp.where(first, b, a), distance, 0)
            for a, b in zip(rows[0::2], rows[1::2])
        ]
    return rows[0]


def aggregate_kernel(
    present_ref, children_ref, interp_ref, phase_ref, out_ref,
    stored, spread, weights_in, phase_in, flags, child_sem, flag_sem, weight_sem, phase_sem,
):
    groups, total = out_ref.shape[:2]
    chunks = total // CHUNK
    span = 4 * LANES * CHUNK
    octants = 8
    parts = 2
    per = 2 * total

    def weight_copy(c):
        at = pl.ds(pl.multiple_of(c * span, span), span)
        return pltpu.make_async_copy(interp_ref.at[:, at], weights_in.at[:, at], weight_sem.at[c])

    def phase_copy(c):
        at = pl.ds(pl.multiple_of(c * span, span), span)
        return pltpu.make_async_copy(phase_ref.at[:, at], phase_in.at[:, at], phase_sem.at[c])

    def child_copy(k):
        at = pl.ds(k * per, per)
        return pltpu.make_async_copy(children_ref.at[at], stored.at[at], child_sem.at[k])

    flag_copy = pltpu.make_async_copy(present_ref, flags, flag_sem)
    flag_copy.start()
    for k in range(parts * octants):
        child_copy(k).start()
    for c in range(chunks):
        weight_copy(c).start()
        phase_copy(c).start()
    flag_copy.wait()

    other = lax.broadcasted_iota(jnp.int32, (8, LANES), 0) ^ 1
    for octant in range(octants):
        flag = flags[0, octant].astype(F32)
        for part in range(parts):
            child_copy(part * octants + octant).wait()

            def unpack(m, carry, flag=flag, octant=octant, part=part):
                at = pl.multiple_of((part * octants + octant) * per + 16 * m, 16)
                rows = stored[pl.ds(at, 16), :].astype(F32) * flag
                to = (part * per + 16 * m) * octants + octant
                for n in range(2):
                    these = rows[8 * n : 8 * n + 8]
                    if octant % 2:
                        these = jnp.take_along_axis(these, other, axis=0, mode="promise_in_bounds")
                    spread[pl.ds(to + 8 * n * octants, 8, stride=octants), :] = these
                return carry

            lax.fori_loop(0, per // 16, unpack, 0, unroll=True)

    lane = lax.broadcasted_iota(jnp.int32, (8, LANES), 1)
    row = lax.broadcasted_iota(jnp.int32, (8, LANES), 0)
    turn = (row - lane // 4) & 7
    row16 = lax.broadcasted_iota(jnp.int32, (16, LANES), 0)
    lane16 = lax.broadcasted_iota(jnp.int32, (16, LANES), 1) // 4
    def bands(first):
        taps = [row16 + 16 * i - first - lane16 for i in range(3)]
        return [jnp.where((tap >= 0) & (tap < 8), 1.0, 0.0).astype(BF16) for tap in taps]

    high_bands, low_bands = bands(0), bands(8)
    lane_16 = lax.broadcasted_iota(jnp.int32, (16, LANES), 1)
    nothing = jnp.zeros((16, LANES), BF16)

    shifts = (HW, HW + AGAIN, LANES // 2 + HW, LANES // 2 + HW + AGAIN - LANES)

    def shifted(index):
        tiles = [
            spread[pl.ds(pl.multiple_of((part * per + 2 * index) * octants, 16), 16), :].astype(BF16)
            for part in range(parts)
        ]
        moved = []
        for tile in tiles:
            near, near_again, far, far_again = (pltpu.roll(tile, shift, 1) for shift in shifts)
            once = lane_16 < AGAIN
            moved.append((jnp.where(once, near, near_again), near_again, jnp.where(once, far, far_again), far_again))
        return moved

    from_before = (lane_16 < HW) | ((lane_16 >= AGAIN) & (lane_16 < AGAIN + HW))
    from_after = (lane_16 >= shifts[2]) & (lane_16 < AGAIN)

    def windows_of(before, now, after):
        first, second = [], []
        for part in range(parts):
            near, near_again, far, far_again = now[part]
            first.append(jnp.concatenate([jnp.where(from_before, before[part][0], near), near_again], axis=1))
            left = jnp.where(from_after, after[part][2], far)
            right = jnp.where(lane_16 < shifts[3], far_again, after[part][3])
            second.append(jnp.concatenate([left, right], axis=1))
        return jnp.concatenate(first, axis=0), jnp.concatenate(second, axis=0)

    def chunk(c, carry):
        weight_copy(c).wait()
        phase_copy(c).wait()
        moved = [shifted(lax.rem(c * CHUNK + i + total, total)) for i in range(-1, CHUNK + 1)]
        for i in range(CHUNK):
            windows = windows_of(*moved[i : i + 3])
            base = pl.multiple_of(c * span, span) + 4 * LANES * i
            real = [None] * 8
            imag = [None] * 8
            for half in range(2):
                high, low = [], []
                for tile in range(2):
                    at = pl.ds(base + (2 * half + tile) * LANES, LANES)
                    turned = jnp.take_along_axis(weights_in[:, at], turn, axis=0, mode="promise_in_bounds")
                    rest = turned - turned.astype(BF16).astype(F32)
                    high.append(jnp.concatenate([turned, turned], axis=0).astype(BF16))
                    low.append(jnp.concatenate([rest, rest], axis=0).astype(BF16))
                left, right = ([part * b for b in high_bands] for part in high)
                left_low, right_low = ([part * b for b in low_bands] for part in low)
                weights = jnp.concatenate(
                    [
                        jnp.concatenate(left + [nothing] + left_low + [nothing] * 9, axis=0),
                        jnp.concatenate([nothing] * 2 + right + [nothing] + right_low + [nothing] * 7, axis=0),
                    ],
                    axis=1,
                )
                refined = jnp.dot(
                    windows[half],
                    weights,
                    preferred_element_type=F32,
                )
                for tile in range(2):
                    at = pl.ds(base + (2 * half + tile) * LANES, LANES)
                    sin_tile, cos_tile = sin_cos(phase_in[:, at])
                    for pol in range(2):
                        re = refined[8 * pol : 8 * pol + 8, tile * LANES : (tile + 1) * LANES]
                        im = refined[16 + 8 * pol : 24 + 8 * pol, tile * LANES : (tile + 1) * LANES]
                        spot = 2 * (2 * half + tile) + pol
                        real[spot] = re * cos_tile - im * sin_tile
                        imag[spot] = re * sin_tile + im * cos_tile
            pattern = jnp.concatenate([row_sums(real), row_sums(imag)], axis=0).astype(BF16)
            for g in range(groups):
                out_ref[g, c * CHUNK + i] = pattern
        return carry

    lax.fori_loop(0, chunks, chunk, 0)


def aggregate(children, present, interp, phase, groups):
    total = children.shape[0] // 32
    chunks = total // CHUNK
    anywhere = pl.BlockSpec(memory_space=pl.ANY)
    return pl.pallas_call(
        aggregate_kernel,
        in_specs=[anywhere, anywhere, anywhere, anywhere],
        out_specs=pl.BlockSpec(memory_space=pltpu.VMEM),
        out_shape=pltpu.VMEM((groups, total, 16, LANES), BF16),
        scratch_shapes=[
            pltpu.VMEM(children.shape, BF16),
            pltpu.VMEM(children.shape, F32),
            pltpu.VMEM(interp.shape, F32),
            pltpu.VMEM(phase.shape, F32),
            pltpu.SMEM(present.shape, jnp.int32),
            pltpu.SemaphoreType.DMA((16,)),
            pltpu.SemaphoreType.DMA,
            pltpu.SemaphoreType.DMA((chunks,)),
            pltpu.SemaphoreType.DMA((chunks,)),
        ],
        compiler_params=pltpu.CompilerParams(vmem_limit_bytes=LIMIT * 1024),
        name="aggregate",
    )(present, children, interp, phase)


def aggregate_local(children, present, interp, phase, groups=2):
    total = children.shape[5] // LANES
    rows = jnp.transpose(children.reshape(2, 8, 2, total, LANES), (0, 1, 3, 2, 4)).reshape(-1, LANES)
    return aggregate(rows, present, interp, phase, groups)


def translate_kernel(
    sources_ref, ids_ref, used_ref, pattern_ref, trans_ref, out_ref, places, table, unpacked, spread_trans, received, table_sem, out_sem
):
    slots, receivers = sources_ref.shape
    clusters = pattern_ref.shape[0] // 16
    batches = receivers // BATCH

    def out_copy(b):
        at = pl.ds(b * BATCH, BATCH)
        return pltpu.make_async_copy(received.at[:, at], out_ref.at[:, at], out_sem.at[b])

    slot_row = lax.broadcasted_iota(jnp.int32, (slots, receivers), 0)
    places[:slots, :] = jnp.where(slot_row < used_ref[...], sources_ref[...], clusters) * 16
    places[slots:, :] = ids_ref[...] * 16
    table_copy = pltpu.make_async_copy(places, table, table_sem)
    table_copy.start()

    def unpack(c, carry):
        at = pl.ds(pl.multiple_of(16 * c, 16), 16)
        unpacked[at, :] = pattern_ref[at, :].astype(F32)
        return carry

    lax.fori_loop(0, clusters, unpack, 0, unroll=8)
    unpacked[pl.ds(16 * clusters, 16), :] = jnp.zeros((16, LANES), F32)
    row = lax.broadcasted_iota(jnp.int32, (8, LANES), 0)
    even = (row & 1) == 0
    order = 2 * (row & 3) + (row >> 2)

    def expand(k, carry):
        operator = trans_ref[pl.ds(pl.multiple_of(8 * k, 8), 8), :]
        at = pl.multiple_of(16 * k, 16)
        spread_trans[pl.ds(at, 8), :] = jnp.where(even, operator, pltpu.roll(operator, 1, 0))
        spread_trans[pl.ds(at + 8, 8), :] = jnp.where(even, pltpu.roll(operator, 7, 0), operator)
        return carry

    lax.fori_loop(0, trans_ref.shape[0] // 8, expand, 0, unroll=4)
    table_copy.wait()

    for receiver in range(receivers):
        real = imag = None
        for slot in range(slots):
            source = pl.multiple_of(table[slot, receiver], 16)
            operator = pl.multiple_of(table[slots + slot, receiver], 16)
            re = unpacked[pl.ds(source, 8), :]
            im = unpacked[pl.ds(source + 8, 8), :]
            t_re = spread_trans[pl.ds(operator, 8), :]
            t_im = spread_trans[pl.ds(operator + 8, 8), :]
            new_re = t_re * re - t_im * im
            new_im = t_re * im + t_im * re
            real = new_re if real is None else real + new_re
            imag = new_im if imag is None else imag + new_im
        received[0, receiver] = jnp.take_along_axis(real, order, axis=0, mode="promise_in_bounds")
        received[1, receiver] = jnp.take_along_axis(imag, order, axis=0, mode="promise_in_bounds")
        if (receiver + 1) % BATCH == 0:
            out_copy(receiver // BATCH).start()
    for b in range(batches):
        out_copy(b).wait()


def translate_local(sources, trans_ids, list_len, pattern, trans):
    kinds = trans.shape[1]
    receivers, slots = sources.shape
    clusters = pattern.shape[0]
    operators = jnp.transpose(
        jnp.transpose(trans, (1, 0, 2)).reshape(kinds, 2, 4, LANES), (0, 2, 1, 3)
    ).reshape(kinds * 8, LANES)
    inside = pl.BlockSpec(memory_space=pltpu.VMEM)
    out = pl.pallas_call(
        translate_kernel,
        in_specs=[inside] * 5,
        out_specs=pl.BlockSpec(memory_space=pl.ANY),
        out_shape=jax.ShapeDtypeStruct((2, receivers, 8, LANES), F32),
        scratch_shapes=[
            pltpu.VMEM((2 * slots, receivers), jnp.int32),
            pltpu.SMEM((2 * slots, receivers), jnp.int32),
            pltpu.VMEM((16 * (clusters + 1), LANES), F32),
            pltpu.VMEM((16 * kinds, LANES), F32),
            pltpu.VMEM((2, receivers, 8, LANES), F32),
            pltpu.SemaphoreType.DMA,
            pltpu.SemaphoreType.DMA((receivers // BATCH,)),
        ],
        compiler_params=pltpu.CompilerParams(vmem_limit_bytes=16 * 2**20),
        name="translate",
    )(sources.T, trans_ids.T, list_len.reshape(1, -1), pattern.reshape(-1, LANES), operators)
    return out.reshape(2, -1, 2, 1, 4 * LANES)


def local(children, present, interp, phase, trans, sources, trans_ids, list_len):
    pattern = aggregate_local(children, present, interp, phase, lax.axis_size("grp"))
    pattern = lax.all_to_all(
        pattern.reshape(-1, 16, LANES), ("grp", "ang"), 0, 0, tiled=True
    )
    return translate_local(sources, trans_ids, list_len, pattern, trans)


def solution(mesh):
    placed = (
        P(None, ("grp", "ang"), None, None, None, None),
        P(("grp", "ang"), None),
        P(),
        P(),
        P(None, None, "ang"),
        P("grp", None),
        P("grp", None),
        P("grp"),
    )
    return jax.shard_map(
        local,
        mesh=mesh,
        in_specs=placed,
        out_specs=P(None, "grp", None, None, "ang"),
        check_vma=False,
    )
```

```python
import functools

import jax
import jax.numpy as jnp
from jax import lax
from jax.experimental import pallas as pl
from jax.experimental.pallas import tpu as pltpu
from jax.sharding import PartitionSpec as P

HW = 4
LANES = 128
CHUNK = 32
AGAIN = 72
LIMIT = 57000
BATCH = 8
F32 = jnp.float32
BF16 = jnp.bfloat16
ROOT = 2.0**0.5

SIN_TERMS = tuple(
    ROOT * v * 0.5 ** (2 * i + 1)
    for i, v in enumerate((1.0, -0.1666666567325592, 0.008333242498338223, -0.00019822783360723406, 2.634888232933008e-06))
)
COS_TERMS = tuple(
    ROOT * v * 0.25**i
    for i, v in enumerate(
        (1.0, -0.5, 0.0416666679084301, -0.0013888812391087413, 2.4786117137409747e-05, -2.6547101583673793e-07)
    )
)


def horner(terms, z):
    total = z * terms[-1] + terms[-2]
    for term in terms[-3::-1]:
        total = total * z + term
    return total


def sin_cos(angle):
    z = angle * angle
    sin_half = angle * horner(SIN_TERMS, z)
    cos_half = horner(COS_TERMS, z)
    return sin_half * cos_half, 1.0 - sin_half * sin_half


def row_sums(rows):
    place = lax.broadcasted_iota(jnp.int32, rows[0].shape, 0)
    rows = [a + pltpu.roll(b, 1, 0) for a, b in zip(rows[0::2], rows[1::2])]
    for distance in (2, 4):
        first = (place & distance) == 0
        rows = [
            jnp.where(first, a, b) + pltpu.roll(jnp.where(first, b, a), distance, 0)
            for a, b in zip(rows[0::2], rows[1::2])
        ]
    return rows[0]


def aggregate_kernel(
    present_ref, children_ref, interp_ref, phase_ref, out_ref,
    stored, spread, weights_in, phase_in, flags, child_sem, flag_sem, weight_sem, phase_sem,
):
    groups, total = out_ref.shape[:2]
    chunks = total // CHUNK
    span = 4 * LANES * CHUNK
    octants = 8
    parts = 2
    per = 2 * total

    def weight_copy(c):
        at = pl.ds(pl.multiple_of(c * span, span), span)
        return pltpu.make_async_copy(interp_ref.at[:, at], weights_in.at[:, at], weight_sem.at[c])

    def phase_copy(c):
        at = pl.ds(pl.multiple_of(c * span, span), span)
        return pltpu.make_async_copy(phase_ref.at[:, at], phase_in.at[:, at], phase_sem.at[c])

    def child_copy(k):
        at = pl.ds(k * per, per)
        return pltpu.make_async_copy(children_ref.at[at], stored.at[at], child_sem.at[k])

    flag_copy = pltpu.make_async_copy(present_ref, flags, flag_sem)
    flag_copy.start()
    for k in range(parts * octants):
        child_copy(k).start()
    for c in range(chunks):
        weight_copy(c).start()
        phase_copy(c).start()
    flag_copy.wait()

    other = lax.broadcasted_iota(jnp.int32, (8, LANES), 0) ^ 1
    for octant in range(octants):
        flag = flags[0, octant].astype(F32)
        for part in range(parts):
            child_copy(part * octants + octant).wait()

            def unpack(m, carry, flag=flag, octant=octant, part=part):
                at = pl.multiple_of((part * octants + octant) * per + 16 * m, 16)
                rows = stored[pl.ds(at, 16), :].astype(F32) * flag
                to = (part * per + 16 * m) * octants + octant
                for n in range(2):
                    these = rows[8 * n : 8 * n + 8]
                    if octant % 2:
                        these = jnp.take_along_axis(these, other, axis=0, mode="promise_in_bounds")
                    spread[pl.ds(to + 8 * n * octants, 8, stride=octants), :] = these
                return carry

            lax.fori_loop(0, per // 16, unpack, 0, unroll=True)

    lane = lax.broadcasted_iota(jnp.int32, (8, LANES), 1)
    row = lax.broadcasted_iota(jnp.int32, (8, LANES), 0)
    turn = (row - lane // 4) & 7
    row16 = lax.broadcasted_iota(jnp.int32, (16, LANES), 0)
    lane16 = lax.broadcasted_iota(jnp.int32, (16, LANES), 1) // 4
    def bands(first):
        taps = [row16 + 16 * i - first - lane16 for i in range(3)]
        return [jnp.where((tap >= 0) & (tap < 8), 1.0, 0.0).astype(BF16) for tap in taps]

    high_bands, low_bands = bands(0), bands(8)
    lane_16 = lax.broadcasted_iota(jnp.int32, (16, LANES), 1)
    nothing = jnp.zeros((16, LANES), BF16)

    shifts = (HW, HW + AGAIN, LANES // 2 + HW, LANES // 2 + HW + AGAIN - LANES)

    def shifted(index):
        tiles = [
            spread[pl.ds(pl.multiple_of((part * per + 2 * index) * octants, 16), 16), :].astype(BF16)
            for part in range(parts)
        ]
        moved = []
        for tile in tiles:
            near, near_again, far, far_again = (pltpu.roll(tile, shift, 1) for shift in shifts)
            once = lane_16 < AGAIN
            moved.append((jnp.where(once, near, near_again), near_again, jnp.where(once, far, far_again), far_again))
        return moved

    from_before = (lane_16 < HW) | ((lane_16 >= AGAIN) & (lane_16 < AGAIN + HW))
    from_after = (lane_16 >= shifts[2]) & (lane_16 < AGAIN)

    def windows_of(before, now, after):
        first, second = [], []
        for part in range(parts):
            near, near_again, far, far_again = now[part]
            first.append(jnp.concatenate([jnp.where(from_before, before[part][0], near), near_again], axis=1))
            left = jnp.where(from_after, after[part][2], far)
            right = jnp.where(lane_16 < shifts[3], far_again, after[part][3])
            second.append(jnp.concatenate([left, right], axis=1))
        return jnp.concatenate(first, axis=0), jnp.concatenate(second, axis=0)

    def chunk(c, carry):
        weight_copy(c).wait()
        phase_copy(c).wait()
        moved = [shifted(lax.rem(c * CHUNK + i + total, total)) for i in range(-1, CHUNK + 1)]
        for i in range(CHUNK):
            windows = windows_of(*moved[i : i + 3])
            base = pl.multiple_of(c * span, span) + 4 * LANES * i
            real = [None] * 8
            imag = [None] * 8
            for half in range(2):
                high, low = [], []
                for tile in range(2):
                    at = pl.ds(base + (2 * half + tile) * LANES, LANES)
                    turned = jnp.take_along_axis(weights_in[:, at], turn, axis=0, mode="promise_in_bounds")
                    rest = turned - turned.astype(BF16).astype(F32)
                    high.append(jnp.concatenate([turned, turned], axis=0).astype(BF16))
                    low.append(jnp.concatenate([rest, rest], axis=0).astype(BF16))
                left, right = ([part * b for b in high_bands] for part in high)
                left_low, right_low = ([part * b for b in low_bands] for part in low)
                weights = jnp.concatenate(
                    [
                        jnp.concatenate(left + [nothing] + left_low + [nothing] * 9, axis=0),
                        jnp.concatenate([nothing] * 2 + right + [nothing] + right_low + [nothing] * 7, axis=0),
                    ],
                    axis=1,
                )
                refined = jnp.dot(
                    windows[half],
                    weights,
                    preferred_element_type=F32,
                )
                for tile in range(2):
                    at = pl.ds(base + (2 * half + tile) * LANES, LANES)
                    sin_tile, cos_tile = sin_cos(phase_in[:, at])
                    for pol in range(2):
                        re = refined[8 * pol : 8 * pol + 8, tile * LANES : (tile + 1) * LANES]
                        im = refined[16 + 8 * pol : 24 + 8 * pol, tile * LANES : (tile + 1) * LANES]
                        spot = 2 * (2 * half + tile) + pol
                        real[spot] = re * cos_tile - im * sin_tile
                        imag[spot] = re * sin_tile + im * cos_tile
            pattern = jnp.concatenate([row_sums(real), row_sums(imag)], axis=0).astype(BF16)
            for g in range(groups):
                out_ref[g, c * CHUNK + i] = pattern
        return carry

    lax.fori_loop(0, chunks, chunk, 0)


def aggregate(children, present, interp, phase, groups):
    total = children.shape[0] // 32
    chunks = total // CHUNK
    anywhere = pl.BlockSpec(memory_space=pl.ANY)
    return pl.pallas_call(
        aggregate_kernel,
        in_specs=[anywhere, anywhere, anywhere, anywhere],
        out_specs=pl.BlockSpec(memory_space=pltpu.VMEM),
        out_shape=pltpu.VMEM((groups, total, 16, LANES), BF16),
        scratch_shapes=[
            pltpu.VMEM(children.shape, BF16),
            pltpu.VMEM(children.shape, F32),
            pltpu.VMEM(interp.shape, F32),
            pltpu.VMEM(phase.shape, F32),
            pltpu.SMEM(present.shape, jnp.int32),
            pltpu.SemaphoreType.DMA((16,)),
            pltpu.SemaphoreType.DMA,
            pltpu.SemaphoreType.DMA((chunks,)),
            pltpu.SemaphoreType.DMA((chunks,)),
        ],
        compiler_params=pltpu.CompilerParams(vmem_limit_bytes=LIMIT * 1024),
        name="aggregate",
    )(present, children, interp, phase)


def aggregate_local(children, present, interp, phase, groups=2):
    total = children.shape[5] // LANES
    rows = jnp.transpose(children.reshape(2, 8, 2, total, LANES), (0, 1, 3, 2, 4)).reshape(-1, LANES)
    return aggregate(rows, present, interp, phase, groups)


def translate_kernel(
    sources_ref, ids_ref, used_ref, pattern_ref, trans_ref, out_ref, places, table, unpacked, spread_trans, received, table_sem, out_sem
):
    slots, receivers = sources_ref.shape
    clusters = pattern_ref.shape[0] // 16
    batches = receivers // BATCH

    def out_copy(b):
        at = pl.ds(b * BATCH, BATCH)
        return pltpu.make_async_copy(received.at[:, at], out_ref.at[:, at], out_sem.at[b])

    slot_row = lax.broadcasted_iota(jnp.int32, (slots, receivers), 0)
    places[:slots, :] = jnp.where(slot_row < used_ref[...], sources_ref[...], clusters) * 16
    places[slots:, :] = ids_ref[...] * 16
    table_copy = pltpu.make_async_copy(places, table, table_sem)
    table_copy.start()

    def unpack(c, carry):
        at = pl.ds(pl.multiple_of(16 * c, 16), 16)
        unpacked[at, :] = pattern_ref[at, :].astype(F32)
        return carry

    lax.fori_loop(0, clusters, unpack, 0, unroll=8)
    unpacked[pl.ds(16 * clusters, 16), :] = jnp.zeros((16, LANES), F32)
    row = lax.broadcasted_iota(jnp.int32, (8, LANES), 0)
    even = (row & 1) == 0
    order = 2 * (row & 3) + (row >> 2)

    def expand(k, carry):
        operator = trans_ref[pl.ds(pl.multiple_of(8 * k, 8), 8), :]
        at = pl.multiple_of(16 * k, 16)
        spread_trans[pl.ds(at, 8), :] = jnp.where(even, operator, pltpu.roll(operator, 1, 0))
        spread_trans[pl.ds(at + 8, 8), :] = jnp.where(even, pltpu.roll(operator, 7, 0), operator)
        return carry

    lax.fori_loop(0, trans_ref.shape[0] // 8, expand, 0, unroll=79)
    table_copy.wait()

    for receiver in range(receivers):
        real = imag = None
        for slot in range(slots):
            source = pl.multiple_of(table[slot, receiver], 16)
            operator = pl.multiple_of(table[slots + slot, receiver], 16)
            re = unpacked[pl.ds(source, 8), :]
            im = unpacked[pl.ds(source + 8, 8), :]
            t_re = spread_trans[pl.ds(operator, 8), :]
            t_im = spread_trans[pl.ds(operator + 8, 8), :]
            new_re = t_re * re - t_im * im
            new_im = t_re * im + t_im * re
            real = new_re if real is None else real + new_re
            imag = new_im if imag is None else imag + new_im
        received[0, receiver] = jnp.take_along_axis(real, order, axis=0, mode="promise_in_bounds")
        received[1, receiver] = jnp.take_along_axis(imag, order, axis=0, mode="promise_in_bounds")
        if (receiver + 1) % BATCH == 0:
            out_copy(receiver // BATCH).start()
    for b in range(batches):
        out_copy(b).wait()


def translate_local(sources, trans_ids, list_len, pattern, trans):
    kinds = trans.shape[1]
    receivers, slots = sources.shape
    clusters = pattern.shape[0]
    operators = jnp.transpose(
        jnp.transpose(trans, (1, 0, 2)).reshape(kinds, 2, 4, LANES), (0, 2, 1, 3)
    ).reshape(kinds * 8, LANES)
    inside = pl.BlockSpec(memory_space=pltpu.VMEM)
    out = pl.pallas_call(
        translate_kernel,
        in_specs=[inside] * 5,
        out_specs=pl.BlockSpec(memory_space=pl.ANY),
        out_shape=jax.ShapeDtypeStruct((2, receivers, 8, LANES), F32),
        scratch_shapes=[
            pltpu.VMEM((2 * slots, receivers), jnp.int32),
            pltpu.SMEM((2 * slots, receivers), jnp.int32),
            pltpu.VMEM((16 * (clusters + 1), LANES), F32),
            pltpu.VMEM((16 * kinds, LANES), F32),
            pltpu.VMEM((2, receivers, 8, LANES), F32),
            pltpu.SemaphoreType.DMA,
            pltpu.SemaphoreType.DMA((receivers // BATCH,)),
        ],
        compiler_params=pltpu.CompilerParams(vmem_limit_bytes=16 * 2**20),
        name="translate",
    )(sources.T, trans_ids.T, list_len.reshape(1, -1), pattern.reshape(-1, LANES), operators)
    return out.reshape(2, -1, 2, 1, 4 * LANES)


def local(children, present, interp, phase, trans, sources, trans_ids, list_len):
    pattern = aggregate_local(children, present, interp, phase, lax.axis_size("grp"))
    pattern = lax.all_to_all(
        pattern.reshape(-1, 16, LANES), ("grp", "ang"), 0, 0, tiled=True
    )
    return translate_local(sources, trans_ids, list_len, pattern, trans)


def solution(mesh):
    placed = (
        P(None, ("grp", "ang"), None, None, None, None),
        P(("grp", "ang"), None),
        P(),
        P(),
        P(None, None, "ang"),
        P("grp", None),
        P("grp", None),
        P("grp"),
    )
    return jax.shard_map(
        local,
        mesh=mesh,
        in_specs=placed,
        out_specs=P(None, "grp", None, None, "ang"),
        check_vma=False,
    )
```
